32 devices in a mesh: rep: 8 (over y, x, core), shard: 4 (over z).
Axes of the slice: x: 2, y: 2, z: 4, core: 2. Of those that a mesh axis runs over, the one named last changes fastest.
Arguments:
- teacher_states: bfloat16 [3072, 5120], P('rep'), may hold values from -16 to 16
- student_states: bfloat16 [3072, 3584], P('rep'), may hold values from -16 to 16
- teacher_gain: float32 [5120], replicated, may hold values from 0.25 to 1.75
- student_gain: float32 [3584], replicated, may hold values from 0.25 to 1.75
- teacher_query: bfloat16 [5120, 3072], P('rep', 'shard'), may hold values from -1 to 1
- teacher_key: bfloat16 [5120, 1024], P('rep', 'shard'), may hold values from -1 to 1
- teacher_value: bfloat16 [5120, 1024], P('rep', 'shard'), may hold values from -0.078125 to 0.078125
- teacher_output: bfloat16 [5120, 3072], P('rep', 'shard'), may hold values from -0.109375 to 0.109375
- student_query: bfloat16 [3584, 2048], P('rep', 'shard'), may hold values from -1 to 1
- student_key: bfloat16 [3584, 512], P('rep'), may hold values from -1 to 1
- student_value: bfloat16 [3584, 512], P('rep'), may hold values from -0.09375 to 0.09375
- student_output: bfloat16 [3584, 2048], P('rep', 'shard'), may hold values from -0.125 to 0.125
- projection: bfloat16 [3584, 5120], P('rep', 'shard'), may hold values from -0.09375 to 0.09375
Outputs:
- query_grad: float32 [3584, 2048], P('rep', 'shard')
- output_grad: float32 [3584, 2048], P('rep', 'shard')
The draws below stay inside these ranges and needn't reach their ends.
All inputs are finite; a program needn't handle non-finite values.
Results may differ from the reference program's by a relative error of at most 0.023.
Values may be sent and summed in bfloat16 or wider, within the bound.
A program may use at most 128 MiB of HBM per device.

```python
import math
from functools import partial
import jax
import jax.numpy as jnp
from jax import lax

D_T = 5120
HQ_T = 24
KV_T = 8
D_S = 3584
HQ_S = 16
KV_S = 4
HD = 128
SEQ = 384
TOKENS = 3072
N_REP = 8
N_SHARD = 4


def weight_matrix(key, label, rows, columns):
    folded = jax.random.fold_in(key, label)
    values = jnp.clip(jax.random.normal(folded, (rows, columns), jnp.float32), -6.0, 6.0)
    return values / math.sqrt(rows)


def drawn_states(key, label, width):
    key_noise = jax.random.fold_in(key, label)
    noise_part = jnp.clip(jax.random.normal(key_noise, (TOKENS, width), jnp.float32), -6.0, 6.0)
    return noise_part


def draw_teacher_states(key, part):
    return drawn_states(key, 11, D_T).astype(jnp.bfloat16)


def draw_student_states(key, part):
    return drawn_states(key, 21, D_S).astype(jnp.bfloat16)


def draw_teacher_query(key, part):
    return weight_matrix(key, 101, D_T, HQ_T * HD).astype(jnp.bfloat16)


def draw_teacher_key(key, part):
    return weight_matrix(key, 102, D_T, KV_T * HD).astype(jnp.bfloat16)


def draw_student_query(key, part):
    return weight_matrix(key, 201, D_S, HQ_S * HD).astype(jnp.bfloat16)


def draw_student_key(key, part):
    return weight_matrix(key, 202, D_S, KV_S * HD).astype(jnp.bfloat16)


def steps_of(key, dims, pieces, low, high):
    def one(dim, shards_of):
        heights = jax.random.uniform(jax.random.fold_in(jax.random.fold_in(key, 6), dim), (shards_of,), jnp.float32, low / len(pieces), high / len(pieces))
        return jnp.repeat(jnp.exp(heights), dims[dim] // shards_of).reshape((-1,) + (1,) * (len(dims) - dim - 1))

    level = one(*pieces[0])
    for cut in pieces[1:]:
        level = level * one(*cut)
    return level


def scatter_about(key, extent, spread, limit, cuts=(), held_as=jnp.bfloat16):
    result = spread * jax.random.normal(key, extent, jnp.float32)
    if cuts:
        result = result * steps_of(key, extent, cuts, -0.22, 0.18)
    return jnp.clip(result, -limit, limit).astype(held_as)


def setup_inputs(seed: int = 0) -> dict:
    key_of = jax.random.split(jax.random.key(seed), 14)
    return {
        "teacher_states": draw_teacher_states(jax.random.fold_in(key_of[13], 71), 0),
        "student_states": draw_student_states(jax.random.fold_in(key_of[13], 71), 0),
        "teacher_gain": jnp.clip(1.0 + 0.15 * jax.random.normal(key_of[2], (D_T,), jnp.float32), 0.25, 1.75),
        "student_gain": jnp.clip(1.0 + 0.15 * jax.random.normal(key_of[3], (D_S,), jnp.float32), 0.25, 1.75),
        "teacher_query": draw_teacher_query(jax.random.fold_in(key_of[13], 71), 0),
        "teacher_key": draw_teacher_key(jax.random.fold_in(key_of[13], 71), 0),
        "teacher_value": scatter_about(key_of[6], (D_T, KV_T * HD), D_T ** -0.5, 0.078125, ((0, 8), (1, 4))),
        "teacher_output": scatter_about(key_of[7], (D_T, HQ_T * HD), (HQ_T * HD) ** -0.5, 0.109375, ((0, 8), (1, 4))),
        "student_query": draw_student_query(jax.random.fold_in(key_of[13], 71), 0),
        "student_key": draw_student_key(jax.random.fold_in(key_of[13], 71), 0),
        "student_value": scatter_about(key_of[10], (D_S, KV_S * HD), D_S ** -0.5, 0.09375, ((0, 8),)),
        "student_output": scatter_about(key_of[11], (D_S, HQ_S * HD), (HQ_S * HD) ** -0.5, 0.125, ((0, 8), (1, 4))),
        "projection": scatter_about(key_of[12], (D_S, D_T), D_S ** -0.5, 0.09375, ((0, 8), (1, 4))),
    }


theta_base = 1000000.0
norm_epsilon = 1e-06

def rms_scale(states, gain):
    values = states.astype(jnp.float32)
    meansq = lax.optimization_barrier(jnp.mean(values * values, axis=-1, keepdims=True))
    return (values * lax.rsqrt(meansq + norm_epsilon) * gain.astype(jnp.float32)).astype(jnp.bfloat16)

def rotate(values, head_dim, turning):
    length = values.shape[0]
    halfway = head_dim // 2
    inverse = theta_base ** (-(jnp.arange(halfway, dtype=jnp.float32) * 2.0 / head_dim))
    angles = jnp.arange(length, dtype=jnp.float32)[:, None] * inverse[None, :]
    cosine = jnp.cos(angles)[:, None, :]
    sine = turning * jnp.sin(angles)[:, None, :]
    split = values.reshape(length, -1, head_dim)
    former = split[..., :halfway]
    latter = split[..., halfway:]
    turned = jnp.concatenate([former * cosine - latter * sine, latter * cosine + former * sine], axis=-1)
    return turned.reshape(length, -1)

def attend(query_rot, keys, values, head_dim):
    length = query_rot.shape[0]
    kv_heads = keys.shape[1] // head_dim
    group_size = query_rot.shape[1] // head_dim // kv_heads
    queries = query_rot.astype(jnp.bfloat16).reshape(length, kv_heads, group_size, head_dim)
    key_heads = keys.reshape(length, kv_heads, head_dim)
    value_heads = values.reshape(length, kv_heads, head_dim)
    scores = jnp.einsum('qkgd,skd->kgqs', queries, key_heads, preferred_element_type=jnp.float32) * head_dim ** (-0.5)
    rows_index = jnp.arange(length)[:, None]
    column_index = jnp.arange(length)[None, :]
    scores = jnp.where(rows_index >= column_index, scores, -1e+30)
    highest = lax.optimization_barrier(jnp.max(scores, axis=-1, keepdims=True))
    weights = jnp.exp(scores - highest)
    probs = (weights / lax.optimization_barrier(jnp.sum(weights, axis=-1, keepdims=True))).astype(jnp.bfloat16)
    mixed = jnp.einsum('kgqs,skd->qkgd', probs, value_heads, preferred_element_type=jnp.float32)
    return mixed.reshape(length, -1)

def block_sum(left, right, blocks):
    length = left.shape[0]
    width = right.shape[0]
    left_blocks = left.reshape(length, blocks, -1)
    right_blocks = right.reshape(width, blocks, -1)
    partials = jnp.einsum('snc,dnc->nsd', left_blocks, right_blocks, preferred_element_type=jnp.float32)
    rounded = lax.optimization_barrier(partials.astype(jnp.bfloat16))
    return lax.optimization_barrier(jnp.sum(rounded.astype(jnp.float32), axis=0))

def reference(teacher_states, student_states, teacher_gain, student_gain, teacher_query, teacher_key, teacher_value, teacher_output, student_query, student_key, student_value, student_output, projection):
    teacher_groups = teacher_states.reshape(N_REP, SEQ, D_T)
    student_groups = student_states.reshape(N_REP, SEQ, D_S)
    scaling = 1.0 / math.sqrt(N_REP * SEQ)

    def one_group(totals, inputs):
        teacher_rows, student_rows = inputs
        normed_t = rms_scale(teacher_rows, teacher_gain)
        query_t = rotate(jnp.dot(normed_t, teacher_query, preferred_element_type=jnp.float32), HD, 1.0)
        keys_t = rotate(jnp.dot(normed_t, teacher_key, preferred_element_type=jnp.float32), HD, 1.0).astype(jnp.bfloat16)
        values_t = jnp.dot(normed_t, teacher_value, preferred_element_type=jnp.float32).astype(jnp.bfloat16)
        mixed_t = attend(query_t, keys_t, values_t, HD).astype(jnp.bfloat16)
        attn_t = block_sum(mixed_t, teacher_output, N_SHARD)
        teacher_hidden = teacher_rows.astype(jnp.float32) + attn_t
        normed_s = rms_scale(student_rows, student_gain)
        query_s = rotate(jnp.dot(normed_s, student_query, preferred_element_type=jnp.float32), HD, 1.0)
        keys_s = rotate(jnp.dot(normed_s, student_key, preferred_element_type=jnp.float32), HD, 1.0).astype(jnp.bfloat16)
        values_s = jnp.dot(normed_s, student_value, preferred_element_type=jnp.float32).astype(jnp.bfloat16)
        mixed_full, pullback = jax.vjp(partial(attend, keys=keys_s, values=values_s, head_dim=HD), query_s)
        mixed_s = mixed_full.astype(jnp.bfloat16)
        attn_s = block_sum(mixed_s, student_output, N_SHARD)
        student_hidden = (student_rows.astype(jnp.float32) + attn_s).astype(jnp.bfloat16)
        predicted = jnp.dot(student_hidden, projection, preferred_element_type=jnp.float32)
        grad_pred = ((predicted - teacher_hidden) * scaling).astype(jnp.bfloat16)
        grad_hidden = block_sum(grad_pred, projection, N_SHARD).astype(jnp.bfloat16)
        out_term = jnp.dot(grad_hidden.T, mixed_s, preferred_element_type=jnp.float32)
        grad_mixed = jnp.dot(grad_hidden, student_output, preferred_element_type=jnp.float32)
        grad_rot = pullback(grad_mixed)[0]
        grad_query = rotate(grad_rot, HD, -1.0).astype(jnp.bfloat16)
        query_term = jnp.dot(normed_s.T, grad_query, preferred_element_type=jnp.float32)
        return ((totals[0] + query_term, totals[1] + out_term), None)
    zeros = jnp.zeros(student_query.shape, jnp.float32)
    (query_total, output_total), _ = lax.scan(one_group, (zeros, zeros), (teacher_groups, student_groups))
    return (query_total, output_total)
```

```python
from functools import partial
import math

import jax
import jax.numpy as jnp
from jax import lax
from jax.experimental import pallas as pl
from jax.experimental.pallas import tpu as pltpu
from jax.sharding import PartitionSpec as P

HQ_S = 16
KV_S = 4
HD = 128

theta_base = 1000000.0
norm_epsilon = 1e-06

F32 = jnp.float32
BF16 = jnp.bfloat16
VMEM_BYTES = 66 * 1000 * 1000
LAG = 2


def tables(length):
    halfway = HD // 2
    inverse = theta_base ** (-(jnp.arange(halfway, dtype=F32) * 2.0 / HD))
    angles = jnp.arange(length, dtype=F32)[:, None] * inverse[None, :]
    cosine = jnp.cos(angles)
    sine = jnp.sin(angles)
    return (
        jnp.concatenate([cosine, cosine], axis=1),
        jnp.concatenate([-sine, sine], axis=1),
    )


def rotate(values, cosine, sine):
    length = values.shape[0]
    split = values.reshape(length, -1, HD)
    swapped = jnp.roll(split, HD // 2, axis=-1)
    turned = split * cosine[:, None, :] + swapped * sine[:, None, :]
    return turned.reshape(length, -1)


def attend(query_rot, keys, values, head_dim):
    length = query_rot.shape[0]
    kv_heads = keys.shape[1] // head_dim
    group_size = query_rot.shape[1] // head_dim // kv_heads
    queries = query_rot.astype(BF16).reshape(length, kv_heads, group_size, head_dim)
    key_heads = keys.reshape(length, kv_heads, head_dim)
    value_heads = values.reshape(length, kv_heads, head_dim)
    scores = jnp.einsum(
        "qkgd,skd->kgqs", queries, key_heads, preferred_element_type=F32
    ) * head_dim ** (-0.5)
    rows_index = jnp.arange(length)[:, None]
    column_index = jnp.arange(length)[None, :]
    scores = jnp.where(rows_index >= column_index, scores, -1e30)
    highest = jnp.max(scores, axis=-1, keepdims=True)
    weights = jnp.exp(scores - highest)
    probs = (weights / jnp.sum(weights, axis=-1, keepdims=True)).astype(BF16)
    mixed = jnp.einsum("kgqs,skd->qkgd", probs, value_heads, preferred_element_type=F32)
    return mixed.reshape(length, -1)


def halving_scatter(term, axis):
    count = lax.axis_size(axis)
    bits = count.bit_length() - 1
    here = lax.axis_index(axis)
    rows = term.shape[0] // count
    width = term.shape[1] // 2
    outs = []
    for half in range(2):
        part = term[:, half * width : (half + 1) * width].reshape((2,) * bits + (rows, width))
        left = list(range(bits - 1, -1, -1))
        order = [0] + (list(range(1, bits)) if half == 0 else list(range(bits - 1, 0, -1)))
        for bit in order:
            place = left.index(bit)
            left.remove(bit)
            mine = lax.rem(lax.div(here, 2**bit), 2)
            sent = lax.dynamic_index_in_dim(part, 1 - mine, place, keepdims=False)
            kept = lax.dynamic_index_in_dim(part, mine, place, keepdims=False)
            came = lax.ppermute(
                sent.astype(BF16), axis, [(i, i ^ (1 << bit)) for i in range(count)]
            )
            part = kept.astype(F32) + came.astype(F32)
        outs.append(part)
    return jnp.concatenate(outs, axis=1)


def tile_of(width):
    return 256 if width % 256 == 0 else 128


def dot_nt(left, right):
    return lax.dot_general(left, right, (((1,), (1,)), ((), ())), preferred_element_type=F32)


class Place:
    def __init__(self, reps, shards):
        self.reps = reps
        self.shards = shards
        self.chips = reps // 2
        self.r = lax.axis_index("rep")
        self.z = lax.axis_index("shard")
        chip = lax.div(self.r, 2)
        self.core = lax.rem(self.r, 2)
        row = lax.div(chip, 2)
        self.pos = 2 * row + lax.rem(lax.rem(chip, 2) + row, 2)
        self.partner = 2 * chip + 1 - self.core
        self.right = self.rep_at(1, self.core)
        self.left = self.rep_at(-1, self.core)

    def rep_at(self, step, core):
        place = lax.rem(self.pos + step + self.chips, self.chips)
        row = lax.div(place, 2)
        chip = 2 * row + lax.rem(lax.rem(place, 2) + row, 2)
        return 2 * chip + core

    def barrier(self, ring, line):
        sem = pltpu.get_barrier_semaphore()
        if ring:
            for target in (self.partner, self.left, self.right):
                pl.semaphore_signal(sem, inc=1, device_id={"rep": target})
        if line:

            @pl.when(self.z > 0)
            def _():
                pl.semaphore_signal(sem, inc=1, device_id={"shard": self.z - 1})

            @pl.when(self.z < self.shards - 1)
            def _():
                pl.semaphore_signal(sem, inc=1, device_id={"shard": self.z + 1})

        peers = 3 if ring else 0
        if line:
            peers += jnp.minimum(self.z, 1) + jnp.minimum(self.shards - 1 - self.z, 1)
        pl.semaphore_wait(sem, peers)


class Gather:
    def __init__(self, place, source, full, index, send_sem, recv_sem, local_sem):
        self.place = place
        self.source = source
        self.full = full
        self.index = index
        self.send_sem = send_sem
        self.recv_sem = recv_sem
        self.local_sem = local_sem
        self.rows = source.shape[0]
        self.half = place.chips // 2

    def slab(self, owner, part):
        if part is None:
            return self.full.at[pl.ds(pl.multiple_of(owner * self.rows, self.rows), self.rows)]
        rows = self.rows // 2
        return self.full.at[pl.ds(pl.multiple_of((2 * owner + part) * rows, rows), rows)]

    def copy(self, message, target, owner, part, source=None):
        slab = self.slab(owner, part)
        return pltpu.make_async_remote_copy(
            src_ref=slab if source is None else source,
            dst_ref=slab,
            send_sem=self.send_sem.at[self.index, message],
            recv_sem=self.recv_sem.at[self.index, message],
            device_id={"rep": target},
        )

    def part_of(self, step, way):
        return None if step < self.half else way

    def local(self):
        return pltpu.make_async_copy(
            self.source, self.slab(self.place.r, None), self.local_sem.at[self.index]
        )

    def start(self):
        p = self.place
        h = self.half
        self.copy(0, p.right, p.r, self.part_of(1, 0), self.source).start()
        self.copy(h, p.left, p.r, self.part_of(1, 1), self.source).start()
        self.copy(2 * h, p.partner, p.r, None, self.source).start()
        self.local().start()

    def relay(self, step):
        p = self.place
        h = self.half
        for way, sign, target in ((0, -1, p.right), (1, 1, p.left)):
            owner = p.rep_at(sign * step, p.core)
            base = way * h
            self.copy(base + step - 1, target, owner, self.part_of(step, way)).wait_recv()
            if step < h:
                self.copy(base + step, target, owner, self.part_of(step + 1, way)).start()
            self.copy(2 * h + base + step, p.partner, owner, self.part_of(step, way)).start()

    def finish(self):
        p = self.place
        h = self.half
        self.local().wait()
        self.copy(2 * h, p.partner, p.partner, None).wait_recv()
        for step in range(1, h + 1):
            for way, sign in ((0, -1), (1, 1)):
                owner = p.rep_at(sign * step, 1 - p.core)
                self.copy(
                    2 * h + way * h + step, p.partner, owner, self.part_of(step, way)
                ).wait_recv()

    def drain(self):
        p = self.place
        h = self.half
        for way, sign, target in ((0, -1, p.right), (1, 1, p.left)):
            for step in range(1, h + 1):
                owner = p.rep_at(sign * (step - 1), p.core)
                self.copy(way * h + step - 1, target, owner, self.part_of(step, way)).wait_send()
                owner = p.rep_at(sign * step, p.core)
                self.copy(
                    2 * h + way * h + step, p.partner, owner, self.part_of(step, way)
                ).wait_send()
        self.copy(2 * h, p.partner, p.r, None).wait_send()


def run_hooks(hooks, wave, last):
    for at, action in hooks:
        if at < last:
            pl.when(wave == at)(action)


def late_hooks(hooks, last):
    for at, action in hooks:
        if at >= last:
            action()


def line_sum(place, count, produce, consume, own, rightward, leftward, send_sem, recv_sem, hooks):
    z = place.z
    ends = place.shards - 1
    waves = count + LAG * ends

    def copy(way, j):
        buffer = (rightward, leftward)[way]
        return pltpu.make_async_remote_copy(
            src_ref=buffer.at[j],
            dst_ref=buffer.at[j],
            send_sem=send_sem.at[way, j],
            recv_sem=recv_sem.at[way, j],
            device_id={"shard": (z + 1, z - 1)[way]},
        )

    def has_before(way):
        return (z > 0, z < ends)[way]

    def has_after(way):
        return (z < ends, z > 0)[way]

    def valid(j):
        return (j >= 0) & (j < count)

    def wave_body(w, carry):
        at = (w - LAG * z, w - LAG * (ends - z))
        first = jnp.maximum(at[0], at[1])
        final = jnp.minimum(at[0], at[1])

        @pl.when(valid(first))
        def _():
            own[first] = produce(first).astype(BF16)

        for way in range(2):
            j = at[way]
            buffer = (rightward, leftward)[way]

            @pl.when(valid(j))
            def _():
                @pl.when(has_before(way))
                def _():
                    copy(way, j).wait_recv()
                    buffer[j] = (own[j].astype(F32) + buffer[j].astype(F32)).astype(BF16)

                @pl.when(jnp.logical_not(has_before(way)))
                def _():
                    buffer[j] = own[j]

                @pl.when(has_after(way))
                def _():
                    copy(way, j).start()

        @pl.when(valid(final))
        def _():
            total = rightward[final].astype(F32) + leftward[final].astype(F32)
            consume(final, total - own[final].astype(F32))

        run_hooks(hooks, w, waves)
        return carry

    lax.fori_loop(0, waves, wave_body, 0)
    late_hooks(hooks, waves)

    def drain(j, carry):
        for way in range(2):

            @pl.when(has_after(way))
            def _():
                copy(way, j).wait_send()

        return carry

    return lambda: lax.fori_loop(0, count, drain, 0)


def line_scatter(place, per_block, produce, own, rightward, leftward, send_sem, recv_sem, hooks):
    z = place.z
    ends = place.shards - 1
    waves = ends * per_block + LAG * ends

    def copy(way, q):
        buffer = (rightward, leftward)[way]
        return pltpu.make_async_remote_copy(
            src_ref=buffer.at[q],
            dst_ref=buffer.at[q],
            send_sem=send_sem.at[way, q],
            recv_sem=recv_sem.at[way, q],
            device_id={"shard": (z + 1, z - 1)[way]},
        )

    def first_own(t, carry):
        own[t] = produce(z * per_block + t).astype(BF16).astype(F32)
        return carry

    lax.fori_loop(0, per_block, first_own, 0)

    def wave_body(w, carry):
        for way in range(2):
            line = (z, ends - z)[way]
            q = w - LAG * line
            past = (ends - line) * per_block
            buffer = (rightward, leftward)[way]
            before = line > 0

            @pl.when((q >= 0) & (q < past))
            def _():
                block = lax.div(q, per_block)
                chunk = lax.rem(q, per_block)
                target = (ends - block, block)[way]
                term = produce(target * per_block + chunk).astype(BF16)

                @pl.when(before)
                def _():
                    copy(way, q).wait_recv()
                    buffer[q] = (term.astype(F32) + buffer[q].astype(F32)).astype(BF16)

                @pl.when(jnp.logical_not(before))
                def _():
                    buffer[q] = term

                copy(way, q).start()

            @pl.when(before & (q >= past) & (q < past + per_block))
            def _():
                copy(way, q).wait_recv()
                own[q - past] += buffer[q].astype(F32)

        run_hooks(hooks, w, waves)
        return carry

    lax.fori_loop(0, waves, wave_body, 0)
    late_hooks(hooks, waves)

    def finish():
        for way in range(2):
            line = (z, ends - z)[way]

            def drain(q, carry):
                copy(way, q).wait_send()
                return carry

            lax.fori_loop(0, (ends - line) * per_block, drain, 0)

    return finish


def normalise(states, gain, block=16):
    length, width = states.shape

    def body(i, carry):
        at = pl.ds(pl.multiple_of(i * block, block), block)
        rows = states[at, :].astype(F32)
        meansq = jnp.sum(rows * rows, axis=-1, keepdims=True) * (1.0 / width)
        states[at, :] = (rows * lax.rsqrt(meansq + norm_epsilon) * gain[...]).astype(BF16)
        return carry

    lax.fori_loop(0, length // block, body, 0)


def turned(values, cosine, sine):
    return values * cosine + pltpu.roll(values, HD // 2, 1) * sine


def project(normed, weight, out, cosine, sine, first, count, tile):
    def body(t, carry):
        at = pl.ds(pl.multiple_of(t * tile, tile), tile)
        value = jnp.dot(normed[...], weight[:, at], preferred_element_type=F32)
        if cosine is None:
            out[:, at] = value.astype(BF16)
        else:
            for head in range(tile // HD):
                part = turned(value[:, head * HD : (head + 1) * HD], cosine[...], sine[...])
                spot = pl.ds(pl.multiple_of(t * tile + head * HD, HD), HD)
                out[:, spot] = part.astype(BF16)
        return carry

    lax.fori_loop(first, first + count, body, 0)


def soft(scores):
    highest = jnp.max(scores, axis=-1, keepdims=True)
    weights = jnp.exp(scores - highest)
    return weights / jnp.sum(weights, axis=-1, keepdims=True)


def masked_scores(query, keys):
    scores = dot_nt(query, keys) * HD ** (-0.5)
    row = lax.broadcasted_iota(jnp.int32, scores.shape, 0)
    column = lax.broadcasted_iota(jnp.int32, scores.shape, 1)
    return jnp.where(row >= column, scores, -1e30)


def attention(queries, keys, values, mixed, first, count, group):
    def body(h, carry):
        at = pl.ds(pl.multiple_of(h * HD, HD), HD)
        kv = pl.ds(pl.multiple_of(lax.div(h, group) * HD, HD), HD)
        probs = soft(masked_scores(queries[:, at], keys[:, kv])).astype(BF16)
        mixed[:, at] = jnp.dot(probs, values[:, kv], preferred_element_type=F32).astype(BF16)
        return carry

    lax.fori_loop(first, first + count, body, 0)


def forward_kernel(
    sizes,
    states_s,
    states_t,
    gain_s,
    gain_t,
    cosine,
    sine,
    w_sq,
    w_sk,
    w_sv,
    w_so,
    w_tq,
    w_tk,
    w_tv,
    w_to,
    w_pj,
    map_full,
    output_full,
    hidden_out,
    attn_out,
    normed_out,
    query_s,
    key_s,
    value_s,
    mixed_s,
    sq,
    sk,
    sv,
    so,
    tq,
    tk,
    tv,
    to,
    normed_s,
    normed_t,
    hidden,
    own_s,
    right_s,
    left_s,
    query_t,
    key_t,
    value_t,
    mixed_t,
    attn_t,
    right_t,
    left_t,
    gather_send,
    gather_recv,
    gather_local,
    sum_send,
    sum_recv,
    scatter_send,
    scatter_recv,
    copies,
):
    reps, shards, kv_start_of = sizes
    place = Place(reps, shards)
    kv_width = sk.shape[1]
    kv_at = pl.ds(pl.multiple_of(kv_start_of(place.z), HD), kv_width)
    sources = (w_sq, w_sk.at[:, kv_at], w_sv.at[:, kv_at], w_so, w_tq, w_tk, w_tv, w_to, w_pj)
    fulls = (sq, sk, sv, so, tq, tk, tv, to, map_full)
    weights = [
        Gather(place, source, full, i, gather_send, gather_recv, gather_local)
        for i, (source, full) in enumerate(zip(sources, fulls))
    ]
    half = place.chips // 2
    groups = {"P0": weights[0:3], "P1": weights[3:4], "P2a": weights[5:7], "P2b": weights[4:5],
              "P3": weights[7:8], "P4": weights[8:9]}

    def start(name):
        for weight in groups[name]:
            weight.start()

    def relay(name, step):
        for weight in groups[name]:
            weight.relay(step)

    def finish(name):
        for step in range(2, half + 1):
            relay(name, step)
        for weight in groups[name]:
            weight.finish()

    in_s = pltpu.make_async_copy(states_s, normed_s, copies.at[0])
    in_h = pltpu.make_async_copy(states_s, hidden, copies.at[1])
    in_t = pltpu.make_async_copy(states_t, normed_t, copies.at[2])
    in_s.start()
    place.barrier(True, True)
    start("P0")
    in_h.start()
    in_t.start()
    in_s.wait()
    normalise(normed_s, gain_s)
    relay("P0", 1)
    start("P1")
    in_t.wait()
    normalise(normed_t, gain_t)
    finish("P0")
    tile = tile_of(sq.shape[1])
    kv_tile = tile_of(kv_width)
    project(normed_s, sk, key_s, cosine, sine, 0, kv_width // kv_tile, kv_tile)
    project(normed_s, sv, value_s, None, None, 0, kv_width // kv_tile, kv_tile)
    project(normed_s, sq, query_s, cosine, sine, 0, sq.shape[1] // tile, tile)
    out_n = pltpu.make_async_copy(normed_s, normed_out, copies.at[3])
    out_n.start()
    relay("P1", 1)
    start("P2a")
    start("P2b")
    heads = sq.shape[1] // HD
    attention(query_s, key_s, value_s, mixed_s, 0, heads, heads // (kv_width // HD))
    finish("P1")
    out_o = pltpu.make_async_copy(so, output_full, copies.at[4])
    out_o.start()
    in_h.wait()

    width = own_s.shape[2]

    def produce_s(j):
        rows = pl.ds(pl.multiple_of(j * width, width), width)
        return dot_nt(mixed_s[...], so[rows, :])

    def consume_s(j, total):
        at = pl.ds(pl.multiple_of(j * width, width), width)
        hidden[:, at] = (hidden[:, at].astype(F32) + total).astype(BF16)

    t_tile = tile_of(tq.shape[1])
    t_kv = tile_of(tk.shape[1])
    t_heads = tq.shape[1] // HD
    t_group = t_heads // (tk.shape[1] // HD)
    hooks = [
        (2, lambda: relay("P2a", 1)),
        (7, lambda: relay("P2b", 1)),
        (7, lambda: start("P3")),
        (9, lambda: finish("P2a")),
        (11, lambda: finish("P2b")),
    ]
    wave = 11
    for t in range(tk.shape[1] // t_kv):
        hooks.append((wave, partial(project, normed_t, tk, key_t, cosine, sine, t, 1, t_kv)))
        hooks.append((wave, partial(project, normed_t, tv, value_t, None, None, t, 1, t_kv)))
        wave += 1
    for t in range(tq.shape[1] // t_tile):
        hooks.append((wave, partial(project, normed_t, tq, query_t, cosine, sine, t, 1, t_tile)))
        wave += 1
    hooks.append((wave, lambda: relay("P3", 1)))
    hooks.append((wave, lambda: start("P4")))
    for h in range(t_heads):
        hooks.append((wave, partial(attention, query_t, key_t, value_t, mixed_t, h, 1, t_group)))
        wave += h % 2
    drain_s = line_sum(
        place, own_s.shape[0], produce_s, consume_s, own_s, right_s, left_s, sum_send, sum_recv, hooks
    )
    out_h = pltpu.make_async_copy(hidden, hidden_out, copies.at[5])
    out_h.start()
    finish("P3")

    width_t = attn_t.shape[2]

    def produce_t(j):
        rows = pl.ds(pl.multiple_of(j * width_t, width_t), width_t)
        return dot_nt(mixed_t[...], to[rows, :])

    drain_t = line_scatter(
        place, attn_t.shape[0], produce_t, attn_t, right_t, left_t, scatter_send, scatter_recv,
        [(3, lambda: relay("P4", 1)), (9, lambda: finish("P4"))],
    )
    out_a = pltpu.make_async_copy(attn_t, attn_out, copies.at[6])
    out_a.start()
    drain_s()
    drain_t()
    for weight in weights:
        weight.drain()
    for copy in (out_n, out_o, out_h, out_a):
        copy.wait()


def gradient_kernel(
    sizes, grad_pred, column_map, hidden_out, map_all, own, right, left, sum_send, sum_recv, copies
):
    reps, shards = sizes
    place = Place(reps, shards)
    inward = pltpu.make_async_copy(column_map, map_all, copies.at[0])
    inward.start()
    place.barrier(False, True)
    inward.wait()
    width = own.shape[2]

    def produce(j):
        rows = pl.ds(pl.multiple_of(j * width, width), width)
        return dot_nt(grad_pred[...], map_all[rows, :])

    def consume(j, total):
        at = pl.ds(pl.multiple_of(j * width, width), width)
        hidden_out[:, at] = total.astype(BF16)

    line_sum(place, own.shape[0], produce, consume, own, right, left, sum_send, sum_recv, [])()


def local(
    reps,
    shards,
    teacher_states,
    student_states,
    teacher_gain,
    student_gain,
    teacher_query,
    teacher_key,
    teacher_value,
    teacher_output,
    student_query,
    student_key,
    student_value,
    student_output,
    projection,
):
    shard_index = lax.axis_index("shard")
    length, d_t = teacher_states.shape
    d_s = student_states.shape[1]
    local_heads = student_query.shape[1] // HD
    group_size = HQ_S // KV_S
    kv_width = max(local_heads // group_size, 1) * HD

    def kv_start_of(z):
        return lax.div(z * local_heads, group_size) * HD

    cosine, sine = tables(length)
    heads_s = student_query.shape[1]
    heads_t = teacher_query.shape[1]
    kv_t = teacher_key.shape[1]
    block_width = projection.shape[1]
    wide_s = tile_of(d_s)
    wide_t = tile_of(block_width)
    count_s = d_s // wide_s
    per_block = block_width // wide_t
    most = (shards - 1) * per_block
    messages = 4 * (reps // 4) + 1
    any_spec = pl.BlockSpec(memory_space=pl.ANY)
    vmem_spec = pl.BlockSpec(memory_space=pltpu.VMEM)
    sds = jax.ShapeDtypeStruct
    dma = pltpu.SemaphoreType.DMA
    column_map, output_full, hidden, attn_block, normed_s, query_rot, keys, values, mixed_s = (
        pl.pallas_call(
            partial(forward_kernel, (reps, shards, kv_start_of)),
            out_shape=(
                sds((d_s, block_width), BF16),
                sds((d_s, heads_s), BF16),
                sds((length, d_s), BF16),
                sds((per_block, length, wide_t), F32),
                sds((length, d_s), BF16),
                sds((length, heads_s), BF16),
                sds((length, kv_width), BF16),
                sds((length, kv_width), BF16),
                sds((length, heads_s), BF16),
            ),
            in_specs=[any_spec] * 2 + [vmem_spec] * 4 + [any_spec] * 9,
            out_specs=(any_spec,) * 5 + (vmem_spec,) * 4,
            scratch_shapes=[
                pltpu.VMEM((d_s, heads_s), BF16),
                pltpu.VMEM((d_s, kv_width), BF16),
                pltpu.VMEM((d_s, kv_width), BF16),
                pltpu.VMEM((d_s, heads_s), BF16),
                pltpu.VMEM((d_t, heads_t), BF16),
                pltpu.VMEM((d_t, kv_t), BF16),
                pltpu.VMEM((d_t, kv_t), BF16),
                pltpu.VMEM((d_t, heads_t), BF16),
                pltpu.VMEM((length, d_s), BF16),
                pltpu.VMEM((length, d_t), BF16),
                pltpu.VMEM((length, d_s), BF16),
                pltpu.VMEM((count_s, length, wide_s), BF16),
                pltpu.VMEM((count_s, length, wide_s), BF16),
                pltpu.VMEM((count_s, length, wide_s), BF16),
                pltpu.VMEM((length, heads_t), BF16),
                pltpu.VMEM((length, kv_t), BF16),
                pltpu.VMEM((length, kv_t), BF16),
                pltpu.VMEM((length, heads_t), BF16),
                pltpu.VMEM((per_block, length, wide_t), F32),
                pltpu.VMEM((most, length, wide_t), BF16),
                pltpu.VMEM((most, length, wide_t), BF16),
                dma((9, messages)),
                dma((9, messages)),
                dma((9,)),
                dma((2, count_s)),
                dma((2, count_s)),
                dma((2, most)),
                dma((2, most)),
                dma((7,)),
            ],
            compiler_params=pltpu.CompilerParams(
                collective_id=0, has_side_effects=True, vmem_limit_bytes=VMEM_BYTES
            ),
        )(
            student_states,
            teacher_states,
            student_gain.reshape(1, -1),
            teacher_gain.reshape(1, -1),
            cosine,
            sine,
            student_query,
            student_key,
            student_value,
            student_output,
            teacher_query,
            teacher_key,
            teacher_value,
            teacher_output,
            projection,
        )
    )
    attn_block = jnp.transpose(attn_block, (1, 0, 2)).reshape(length, block_width)
    own_states = lax.dynamic_slice_in_dim(teacher_states, shard_index * block_width, block_width, 1)
    teacher_hidden = own_states.astype(F32) + attn_block
    scaling = 1.0 / math.sqrt(reps * length)
    predicted = jnp.dot(hidden, column_map, preferred_element_type=F32)
    grad_pred = ((predicted - teacher_hidden) * scaling).astype(BF16)
    grad_hidden = pl.pallas_call(
        partial(gradient_kernel, (reps, shards)),
        out_shape=sds((length, d_s), BF16),
        in_specs=[vmem_spec, any_spec],
        out_specs=vmem_spec,
        scratch_shapes=[
            pltpu.VMEM((d_s, block_width), BF16),
            pltpu.VMEM((count_s, length, wide_s), BF16),
            pltpu.VMEM((count_s, length, wide_s), BF16),
            pltpu.VMEM((count_s, length, wide_s), BF16),
            dma((2, count_s)),
            dma((2, count_s)),
            dma((1,)),
        ],
        compiler_params=pltpu.CompilerParams(
            collective_id=1, has_side_effects=True, vmem_limit_bytes=VMEM_BYTES
        ),
    )(grad_pred, column_map)
    grad_mixed = jnp.dot(grad_hidden, output_full, preferred_element_type=F32)
    _, pullback = jax.vjp(
        partial(attend, keys=keys, values=values, head_dim=HD), query_rot.astype(F32)
    )
    grad_rot = pullback(grad_mixed)[0]
    grad_query = rotate(grad_rot, cosine, -sine).astype(BF16)
    out_term = jnp.dot(grad_hidden.T, mixed_s, preferred_element_type=F32)
    query_term = jnp.dot(normed_s.T, grad_query, preferred_element_type=F32)
    return (halving_scatter(query_term, "rep"), halving_scatter(out_term, "rep"))


def solution(mesh):
    return jax.shard_map(
        partial(local, mesh.shape["rep"], mesh.shape["shard"]),
        mesh=mesh,
        in_specs=(
            P("rep", None),
            P("rep", None),
            P(),
            P(),
            P("rep", "shard"),
            P("rep", "shard"),
            P("rep", "shard"),
            P("rep", "shard"),
            P("rep", "shard"),
            P("rep", None),
            P("rep", None),
            P("rep", "shard"),
            P("rep", "shard"),
        ),
        out_specs=(P("rep", "shard"), P("rep", "shard")),
        check_vma=False,
    )
```

```python
from functools import partial
import math

import jax
import jax.numpy as jnp
import numpy as np
from jax import lax
from jax.experimental import pallas as pl
from jax.experimental.pallas import tpu as pltpu
from jax.sharding import PartitionSpec as P

HQ_S = 16
KV_S = 4
HD = 128

theta_base = 1000000.0
norm_epsilon = 1e-06

F32 = jnp.float32
BF16 = jnp.bfloat16
VMEM_BYTES = 67_000_000
LAG = 2


def tables(length):
    halfway = HD // 2
    inverse = theta_base ** (-(np.arange(halfway) * 2.0 / HD))
    inverse = inverse.astype(np.float32)
    angles = np.arange(length, dtype=np.float32)[:, None] * inverse[None, :]
    cosine = np.cos(angles)
    sine = np.sin(angles)
    return (
        np.concatenate([cosine, cosine], axis=1).astype(np.float32),
        np.concatenate([-sine, sine], axis=1).astype(np.float32),
    )


def tile_of(width):
    return 256 if width % 256 == 0 else 128


def dot_nt(left, right):
    return lax.dot_general(left, right, (((1,), (1,)), ((), ())), preferred_element_type=F32)


def dot_tn(left, right):
    return lax.dot_general(left, right, (((0,), (0,)), ((), ())), preferred_element_type=F32)


def span(index, size):
    return pl.ds(pl.multiple_of(index * size, size), size)


class Place:
    def __init__(self, reps, shards):
        self.reps = reps
        self.shards = shards
        self.chips = reps // 2
        self.r = lax.axis_index("rep")
        self.z = lax.axis_index("shard")
        chip = lax.div(self.r, 2)
        self.core = lax.rem(self.r, 2)
        row = lax.div(chip, 2)
        self.pos = 2 * row + lax.rem(lax.rem(chip, 2) + row, 2)
        self.partner = 2 * chip + 1 - self.core
        self.right = self.rep_at(1, self.core)
        self.left = self.rep_at(-1, self.core)

    def rep_at(self, step, core):
        place = lax.rem(self.pos + step + self.chips, self.chips)
        row = lax.div(place, 2)
        chip = 2 * row + lax.rem(lax.rem(place, 2) + row, 2)
        return 2 * chip + core

    def barrier(self, ring, line):
        sem = pltpu.get_barrier_semaphore()
        if ring:
            for target in (self.partner, self.left, self.right):
                pl.semaphore_signal(sem, inc=1, device_id={"rep": target})
        if line:

            @pl.when(self.z > 0)
            def _():
                pl.semaphore_signal(sem, inc=1, device_id={"shard": self.z - 1})

            @pl.when(self.z < self.shards - 1)
            def _():
                pl.semaphore_signal(sem, inc=1, device_id={"shard": self.z + 1})

        peers = 3 if ring else 0
        if line:
            peers += jnp.minimum(self.z, 1) + jnp.minimum(self.shards - 1 - self.z, 1)
        pl.semaphore_wait(sem, peers)


class Gather:
    def __init__(self, place, source, full, index, send_sem, recv_sem, local_sem):
        self.place = place
        self.source = source
        self.full = full
        self.index = index
        self.send_sem = send_sem
        self.recv_sem = recv_sem
        self.local_sem = local_sem
        self.rows = source.shape[0]
        self.half = place.chips // 2

    def slab(self, owner, part):
        if part is None:
            return self.full.at[pl.ds(pl.multiple_of(owner * self.rows, self.rows), self.rows)]
        rows = self.rows // 2
        return self.full.at[pl.ds(pl.multiple_of((2 * owner + part) * rows, rows), rows)]

    def copy(self, message, target, owner, part, source=None):
        slab = self.slab(owner, part)
        return pltpu.make_async_remote_copy(
            src_ref=slab if source is None else source,
            dst_ref=slab,
            send_sem=self.send_sem.at[self.index, message],
            recv_sem=self.recv_sem.at[self.index, message],
            device_id={"rep": target},
        )

    def part_of(self, step, way):
        return None if step < self.half else way

    def local(self):
        return pltpu.make_async_copy(
            self.source, self.slab(self.place.r, None), self.local_sem.at[self.index]
        )

    def start(self):
        p = self.place
        h = self.half
        self.copy(0, p.right, p.r, self.part_of(1, 0), self.source).start()
        self.copy(h, p.left, p.r, self.part_of(1, 1), self.source).start()
        self.copy(2 * h, p.partner, p.r, None, self.source).start()
        self.local().start()

    def relay(self, step):
        p = self.place
        h = self.half
        for way, sign, target in ((0, -1, p.right), (1, 1, p.left)):
            owner = p.rep_at(sign * step, p.core)
            base = way * h
            self.copy(base + step - 1, target, owner, self.part_of(step, way)).wait_recv()
            if step < h:
                self.copy(base + step, target, owner, self.part_of(step + 1, way)).start()
            self.copy(2 * h + base + step, p.partner, owner, self.part_of(step, way)).start()

    def finish(self):
        p = self.place
        h = self.half
        self.local().wait()
        self.copy(2 * h, p.partner, p.partner, None).wait_recv()
        for step in range(1, h + 1):
            for way, sign in ((0, -1), (1, 1)):
                owner = p.rep_at(sign * step, 1 - p.core)
                self.copy(
                    2 * h + way * h + step, p.partner, owner, self.part_of(step, way)
                ).wait_recv()

    def drain(self):
        p = self.place
        h = self.half
        for way, sign, target in ((0, -1, p.right), (1, 1, p.left)):
            for step in range(1, h + 1):
                owner = p.rep_at(sign * (step - 1), p.core)
                self.copy(way * h + step - 1, target, owner, self.part_of(step, way)).wait_send()
                owner = p.rep_at(sign * step, p.core)
                self.copy(
                    2 * h + way * h + step, p.partner, owner, self.part_of(step, way)
                ).wait_send()
        self.copy(2 * h, p.partner, p.r, None).wait_send()


def run_hooks(hooks, wave, last):
    for at, action in hooks:
        if at < last:
            pl.when(wave == at)(action)


def late_hooks(hooks, last):
    for at, action in hooks:
        if at >= last:
            action()


def line_sum(place, count, produce, consume, own, rightward, leftward, send_sem, recv_sem, hooks,
             done_hooks=()):
    z = place.z
    ends = place.shards - 1
    waves = count + LAG * ends

    def copy(way, j):
        buffer = (rightward, leftward)[way]
        return pltpu.make_async_remote_copy(
            src_ref=buffer.at[j],
            dst_ref=buffer.at[j],
            send_sem=send_sem.at[way, j],
            recv_sem=recv_sem.at[way, j],
            device_id={"shard": (z + 1, z - 1)[way]},
        )

    def has_before(way):
        return (z > 0, z < ends)[way]

    def has_after(way):
        return (z < ends, z > 0)[way]

    def valid(j):
        return (j >= 0) & (j < count)

    def wave_body(w, carry):
        at = (w - LAG * z, w - LAG * (ends - z))
        first = jnp.maximum(at[0], at[1])
        final = jnp.minimum(at[0], at[1])

        @pl.when(valid(first))
        def _():
            own[first] = produce(first).astype(BF16)

        for way in range(2):
            j = at[way]
            buffer = (rightward, leftward)[way]

            @pl.when(valid(j))
            def _():
                @pl.when(has_before(way))
                def _():
                    copy(way, j).wait_recv()
                    buffer[j] = (own[j].astype(F32) + buffer[j].astype(F32)).astype(BF16)

                @pl.when(jnp.logical_not(has_before(way)))
                def _():
                    buffer[j] = own[j]

                @pl.when(has_after(way))
                def _():
                    copy(way, j).start()

        @pl.when(valid(final))
        def _():
            total = rightward[final].astype(F32) + leftward[final].astype(F32)
            consume(final, total - own[final].astype(F32))
            run_hooks(done_hooks, final, count)

        run_hooks(hooks, w, waves)
        return carry

    lax.fori_loop(0, waves, wave_body, 0)
    late_hooks(hooks, waves)
    late_hooks(done_hooks, count)

    def drain(j, carry):
        for way in range(2):

            @pl.when(has_after(way))
            def _():
                copy(way, j).wait_send()

        return carry

    return lambda: lax.fori_loop(0, count, drain, 0)


def line_scatter(place, per_block, produce, own, rightward, leftward, send_sem, recv_sem, hooks):
    z = place.z
    ends = place.shards - 1
    waves = ends * per_block + LAG * ends

    def copy(way, q):
        buffer = (rightward, leftward)[way]
        return pltpu.make_async_remote_copy(
            src_ref=buffer.at[q],
            dst_ref=buffer.at[q],
            send_sem=send_sem.at[way, q],
            recv_sem=recv_sem.at[way, q],
            device_id={"shard": (z + 1, z - 1)[way]},
        )

    def first_own(t, carry):
        own[t] = produce(z * per_block + t).astype(BF16).astype(F32)
        return carry

    lax.fori_loop(0, per_block, first_own, 0)

    def wave_body(w, carry):
        for way in range(2):
            line = (z, ends - z)[way]
            q = w - LAG * line
            past = (ends - line) * per_block
            buffer = (rightward, leftward)[way]
            before = line > 0

            @pl.when((q >= 0) & (q < past))
            def _():
                block = lax.div(q, per_block)
                chunk = lax.rem(q, per_block)
                target = (ends - block, block)[way]
                term = produce(target * per_block + chunk).astype(BF16)

                @pl.when(before)
                def _():
                    copy(way, q).wait_recv()
                    buffer[q] = (term.astype(F32) + buffer[q].astype(F32)).astype(BF16)

                @pl.when(jnp.logical_not(before))
                def _():
                    buffer[q] = term

                copy(way, q).start()

            @pl.when(before & (q >= past) & (q < past + per_block))
            def _():
                copy(way, q).wait_recv()
                own[q - past] += buffer[q].astype(F32)

        run_hooks(hooks, w, waves)
        return carry

    lax.fori_loop(0, waves, wave_body, 0)
    late_hooks(hooks, waves)

    def finish():
        for way in range(2):
            line = (z, ends - z)[way]

            def drain(q, carry):
                copy(way, q).wait_send()
                return carry

            lax.fori_loop(0, (ends - line) * per_block, drain, 0)

    return finish


class RingScatter:
    def __init__(self, place, partial_sums, pair, ring, out, index, pair_sems, ring_sems):
        self.place = place
        self.partial = partial_sums
        self.pair = pair
        self.ring = ring
        self.out = out
        self.index = index
        self.pair_sems = pair_sems
        self.ring_sems = ring_sems
        self.half = place.chips // 2
        self.rows = out.shape[0]
        self.steps = ring_order(place.chips)

    def exchange(self, i):
        self.pair_copy(i).start()

    def pair_copy(self, i):
        owner = self.place.rep_at(self.steps[i], 1 - self.place.core)
        return pltpu.make_async_remote_copy(
            src_ref=self.partial.at[span(owner, self.rows)],
            dst_ref=self.pair(i),
            send_sem=self.pair_sems[0].at[self.index, i],
            recv_sem=self.pair_sems[1].at[self.index, i],
            device_id={"rep": self.place.partner},
        )

    def message(self, step, part):
        return 0 if step == self.half else 1 + 2 * (self.half - 1 - step) + part

    def half_of(self, ref, part):
        return ref.at[pl.ds(part * (self.rows // 2), self.rows // 2)]

    def ring_copy(self, way, step, part, i):
        m = self.message(step, part)
        return pltpu.make_async_remote_copy(
            src_ref=self.half_of(self.pair(i), part),
            dst_ref=self.ring.at[way, m],
            send_sem=self.ring_sems[0].at[self.index, way, m],
            recv_sem=self.ring_sems[1].at[self.index, way, m],
            device_id={"rep": (self.place.right, self.place.left)[way]},
        )

    def moves(self, i):
        e, h = self.steps[i], self.half
        if e == h:
            return [(way, h, way, False) for way in range(2)]
        way, step = (0, e) if e > 0 else (1, -e)
        return [(way, step, part, part == way or step + 1 < h) for part in range(2)]

    def fresh(self, i, part):
        owner = self.place.rep_at(self.steps[i], self.place.core)
        rows = self.rows // 2
        mine = self.partial[span(2 * owner + part, rows), :].astype(F32)
        return mine + self.half_of(self.pair(i), part)[...].astype(F32)

    def incoming(self, way, step, part, i):
        self.ring_copy(way, step, part, i).wait_recv()
        return self.ring[way, self.message(step, part)].astype(F32)

    def forward(self, i):
        self.pair_copy(i).wait_recv()
        if self.steps[i] != 0:
            for way, step, part, has in self.moves(i):
                value = self.fresh(i, part)
                if has:
                    value = value + self.incoming(way, step + 1, part, i)
                self.half_of(self.pair(i), part)[...] = value.astype(BF16)
                self.ring_copy(way, step, part, i).start()
            return
        for part in range(2):
            value = self.fresh(i, part)
            for way in range(2):
                if part == way or self.half > 1:
                    value = value + self.incoming(way, 1, part, i)
            self.half_of(self.out, part)[...] = value

    def drain(self):
        for i, e in enumerate(self.steps):
            self.pair_copy(i).wait_send()
            if e != 0:
                for way, step, part, _ in self.moves(i):
                    self.ring_copy(way, step, part, i).wait_send()


def ring_order(chips):
    half = chips // 2
    order = [half]
    for step in range(half - 1, 0, -1):
        order += [step, -step]
    return order + [0]


def normalise(states, gain, block=16):
    length, width = states.shape

    def body(i, carry):
        at = pl.ds(pl.multiple_of(i * block, block), block)
        rows = states[at, :].astype(F32)
        meansq = jnp.sum(rows * rows, axis=-1, keepdims=True) * (1.0 / width)
        states[at, :] = (rows * lax.rsqrt(meansq + norm_epsilon) * gain[...]).astype(BF16)
        return carry

    lax.fori_loop(0, length // block, body, 0)


def turned(values, cosine, sine):
    return values * cosine + pltpu.roll(values, HD // 2, 1) * sine


def project(normed, weight, out, cosine, sine, first, count, tile):
    def body(t, carry):
        at = pl.ds(pl.multiple_of(t * tile, tile), tile)
        value = jnp.dot(normed[...], weight[:, at], preferred_element_type=F32)
        if cosine is None:
            out[:, at] = value.astype(BF16)
        else:
            for head in range(tile // HD):
                part = turned(value[:, head * HD : (head + 1) * HD], cosine[...], sine[...])
                spot = pl.ds(pl.multiple_of(t * tile + head * HD, HD), HD)
                out[:, spot] = part.astype(BF16)
        return carry

    lax.fori_loop(first, first + count, body, 0)


def soft(scores):
    highest = jnp.max(scores, axis=-1, keepdims=True)
    weights = jnp.exp(scores - highest)
    return weights / jnp.sum(weights, axis=-1, keepdims=True)


def masked_scores(query, keys):
    scores = dot_nt(query, keys) * HD ** (-0.5)
    row = lax.broadcasted_iota(jnp.int32, scores.shape, 0)
    column = lax.broadcasted_iota(jnp.int32, scores.shape, 1)
    return jnp.where(row >= column, scores, -1e30)


def attention(queries, keys, values, mixed, first, count, group):
    def body(h, carry):
        at = pl.ds(pl.multiple_of(h * HD, HD), HD)
        kv = pl.ds(pl.multiple_of(lax.div(h, group) * HD, HD), HD)
        probs = soft(masked_scores(queries[:, at], keys[:, kv])).astype(BF16)
        mixed[:, at] = jnp.dot(probs, values[:, kv], preferred_element_type=F32).astype(BF16)
        return carry

    lax.fori_loop(first, first + count, body, 0)


def backward_head(h, query, keys, values, grad_mixed, grad_query, cosine, sine, group):
    at = span(h, HD)
    kv = span(lax.div(h, group), HD)
    probs = soft(masked_scores(query[:, at], keys[:, kv]))
    grad_probs = dot_nt(grad_mixed[:, at].astype(BF16), values[:, kv]).astype(BF16).astype(F32)
    inner = jnp.sum(grad_probs * probs, axis=-1, keepdims=True)
    grad_scores = probs * (grad_probs - inner) * HD ** (-0.5)
    grad_rot = jnp.dot(grad_scores.astype(BF16), keys[:, kv], preferred_element_type=F32)
    grad_rot = grad_rot.astype(BF16).astype(F32)
    grad_query[:, at] = turned(grad_rot, cosine[...], -sine[...]).astype(BF16)


def step_kernel(
    sizes,
    states_s,
    states_t,
    gain_s,
    gain_t,
    cosine,
    sine,
    w_sq,
    w_sk,
    w_sv,
    w_so,
    w_tq,
    w_tk,
    w_tv,
    w_to,
    w_pj,
    map_full,
    query_grad,
    output_grad,
    sq,
    sk,
    sv,
    so,
    tq,
    tk,
    tv,
    to,
    normed_s,
    normed_t,
    hidden,
    own_s,
    right_s,
    left_s,
    query_s,
    key_s,
    value_s,
    mixed_s,
    query_t,
    key_t,
    value_t,
    mixed_t,
    attn_t,
    right_t,
    left_t,
    grad_mixed,
    ring_out,
    ring_query,
    gather_send,
    gather_recv,
    gather_local,
    sum_send,
    sum_recv,
    back_send,
    back_recv,
    scatter_send,
    scatter_recv,
    pair_send,
    pair_recv,
    ring_send,
    ring_recv,
    copies,
    map_sems,
):
    reps, shards, kv_start_of = sizes
    place = Place(reps, shards)
    length = normed_s.shape[0]
    kv_width = sk.shape[1]
    kv_at = pl.ds(pl.multiple_of(kv_start_of(place.z), HD), kv_width)
    sources = (w_sq, w_sk.at[:, kv_at], w_sv.at[:, kv_at], w_so, w_tq, w_tk, w_tv, w_to, w_pj)
    fulls = (sq, sk, sv, so, tq, tk, tv, to, map_full)
    weights = [
        Gather(place, source, full, i, gather_send, gather_recv, gather_local)
        for i, (source, full) in enumerate(zip(sources, fulls))
    ]
    half = place.chips // 2
    groups = {
        "P0": weights[0:3],
        "P1": weights[3:4],
        "P2a": weights[5:7],
        "P2b": weights[4:5],
        "P3": weights[7:8],
        "P4": weights[8:9],
    }

    def start(name):
        for weight in groups[name]:
            weight.start()

    def relay(name, step):
        for weight in groups[name]:
            weight.relay(step)

    def finish(name):
        for step in range(2, half + 1):
            relay(name, step)
        for weight in groups[name]:
            weight.finish()

    def drain(names):
        for name in names:
            for weight in groups[name]:
                weight.drain()

    in_s = pltpu.make_async_copy(states_s, normed_s, copies.at[0])
    in_h = pltpu.make_async_copy(states_s, hidden, copies.at[1])
    in_t = pltpu.make_async_copy(states_t, normed_t, copies.at[2])
    in_s.start()
    place.barrier(True, True)
    start("P0")
    in_h.start()
    in_t.start()
    in_s.wait()
    normalise(normed_s, gain_s)
    relay("P0", 1)
    start("P1")
    in_t.wait()
    normalise(normed_t, gain_t)
    finish("P0")
    tile = tile_of(sq.shape[1])
    kv_tile = tile_of(kv_width)
    project(normed_s, sk, key_s, cosine, sine, 0, kv_width // kv_tile, kv_tile)
    project(normed_s, sv, value_s, None, None, 0, kv_width // kv_tile, kv_tile)
    project(normed_s, sq, query_s, cosine, sine, 0, sq.shape[1] // tile, tile)
    relay("P1", 1)
    start("P2a")
    start("P2b")
    heads = sq.shape[1] // HD
    group = heads // (kv_width // HD)
    attention(query_s, key_s, value_s, mixed_s, 0, heads, group)
    finish("P1")
    in_h.wait()

    count, _, width = own_s.shape
    block_width = map_full.shape[1]
    states_at = pl.ds(pl.multiple_of(place.z * block_width, 128), block_width)
    in_b = pltpu.make_async_copy(
        states_t.at[:, states_at], normed_t.at[:, 0:block_width], copies.at[3]
    )

    def produce_s(j):
        return dot_nt(mixed_s[...], so[span(j, width), :])

    def consume_s(j, total):
        at = span(j, width)
        hidden[:, at] = (hidden[:, at].astype(F32) + total).astype(BF16)

    t_tile = tile_of(tq.shape[1])
    t_kv = tile_of(tk.shape[1])
    t_heads = tq.shape[1] // HD
    t_group = t_heads // (tk.shape[1] // HD)
    hooks = [
        (5, lambda: relay("P2a", 1)),
        (14, lambda: relay("P2b", 1)),
        (14, lambda: start("P3")),
        (17, lambda: finish("P2a")),
        (22, lambda: finish("P2b")),
    ]
    wave = 22
    for t in range(tk.shape[1] // t_kv):
        hooks.append((wave, partial(project, normed_t, tk, key_t, cosine, sine, t, 1, t_kv)))
        wave += 1
        hooks.append((wave, partial(project, normed_t, tv, value_t, None, None, t, 1, t_kv)))
        wave += 1
    for t in range(tq.shape[1] // t_tile):
        hooks.append((wave, partial(project, normed_t, tq, query_t, cosine, sine, t, 1, t_tile)))
        wave += 1
    hooks.append((wave, lambda: drain(("P0", "P1", "P2a", "P2b"))))
    hooks.append((wave, in_b.start))
    for h in range(t_heads):
        hooks.append((wave, partial(attention, query_t, key_t, value_t, mixed_t, h, 1, t_group)))
        wave += 1
    hooks.append((wave - 2, lambda: relay("P3", 1)))
    hooks.append((wave - 2, lambda: start("P4")))
    drain_s = line_sum(
        place, count, produce_s, consume_s, own_s, right_s, left_s, sum_send, sum_recv, hooks
    )
    drain_s()
    finish("P3")

    per_block, _, width_t = attn_t.shape
    in_b.wait()

    def produce_t(j):
        return dot_nt(mixed_t[...], to[span(j, width_t), :])

    columns = (tk, tv)

    def column_copy(t):
        return pltpu.make_async_copy(
            map_full.at[:, t * width_t : (t + 1) * width_t],
            columns[t % 2].at[0 : map_full.shape[0]],
            map_sems.at[t % 2],
        )

    def first_columns():
        for t in range(min(2, per_block)):
            column_copy(t).start()

    def predict(t):
        column_copy(t).wait()
        product = jnp.dot(
            hidden[...], columns[t % 2][0 : map_full.shape[0]], preferred_element_type=F32
        )
        at = pl.ds(t * width_t, width_t)
        attn_t[t] += normed_t[:, at].astype(F32) - product
        if t + 2 < per_block:
            column_copy(t + 2).start()

    hooks = [(2, lambda: relay("P4", 1)), (8, lambda: finish("P4")), (8, first_columns)]
    hooks += [(9 + t, partial(predict, t)) for t in range(per_block)]
    drain_t = line_scatter(
        place, per_block, produce_t, attn_t, right_t, left_t, scatter_send, scatter_recv, hooks
    )
    scaling = 1.0 / math.sqrt(reps * length)
    grad_pred = normed_t.at[:, 0:block_width]
    for t in range(per_block):
        grad_pred[:, t * width_t : (t + 1) * width_t] = (attn_t[t] * -scaling).astype(BF16)

    rows = query_grad.shape[0]
    wide = query_grad.shape[1]
    pair_sems = (pair_send, pair_recv)
    ring_sems = (ring_send, ring_recv)

    def slot(first):
        return lambda i: tq.at[(first + i) * rows : (first + i + 1) * rows, 0:wide]

    out_sum = RingScatter(
        place, sq, slot(0), ring_out, output_grad, 0, pair_sems, ring_sems
    )
    query_sum = RingScatter(
        place, so, slot(place.chips), ring_query, query_grad, 1, pair_sems, ring_sems
    )
    steps = ring_order(place.chips)
    per_chip = count // place.chips
    in_order = per_chip * place.chips == count

    def tile_at(j):
        if not in_order:
            return j
        turn = lax.div(j, per_chip)
        chip = 0
        for i, step in enumerate(steps):
            chip = chip + jnp.where(turn == i, lax.div(place.rep_at(step, 0), 2), 0)
        return chip * per_chip + lax.rem(j, per_chip)

    slots = length // width

    def rows_copy(j):
        slot_at = lax.rem(j, slots)
        return pltpu.make_async_copy(
            map_full.at[span(tile_at(j), width)],
            normed_t.at[span(slot_at, width), block_width : 2 * block_width],
            map_sems.at[2 + slot_at],
        )

    def produce_b(j):
        rows_copy(j).wait()
        at = span(lax.rem(j, slots), width)
        product = dot_nt(grad_pred[...], normed_t[at, block_width : 2 * block_width])

        @pl.when(j + slots < count)
        def _():
            rows_copy(j + slots).start()

        return product

    grad_mixed[...] = jnp.zeros_like(grad_mixed)

    def consume_b(j, total):
        at = span(tile_at(j), width)
        grad = total.astype(BF16)
        grad_mixed[...] += jnp.dot(grad, so[at, :], preferred_element_type=F32)
        sq[at, :] = dot_tn(grad, mixed_s[...]).astype(BF16)

    for j in range(min(slots, count)):
        rows_copy(j).start()
    done = []
    for i in range(place.chips):
        ready = (i + 1) * per_chip - 1 if in_order else count
        done.append((ready, partial(out_sum.exchange, i)))
        done.append((ready + 3 if in_order else count, partial(out_sum.forward, i)))
    drain_b = line_sum(
        place, count, produce_b, consume_b, own_s, right_s, left_s, back_send, back_recv, [], done
    )
    grad_query = query_t.at[:, 0:wide]

    def one_head(h, carry):
        backward_head(h, query_s, key_s, value_s, grad_mixed, grad_query, cosine, sine, group)
        return carry

    lax.fori_loop(0, heads, one_head, 0)

    def query_tile(t, carry):
        so[span(t, width), :] = dot_tn(normed_s[:, span(t, width)], grad_query[...]).astype(BF16)
        return carry

    if in_order:
        for i, step in enumerate(steps):
            first = lax.div(place.rep_at(step, 0), 2) * per_chip
            lax.fori_loop(first, first + per_chip, query_tile, 0)
            query_sum.exchange(i)
            if i > 0:
                query_sum.forward(i - 1)
        query_sum.forward(len(steps) - 1)
    else:
        lax.fori_loop(0, count, query_tile, 0)
        for i in range(len(steps)):
            query_sum.exchange(i)
        for i in range(len(steps)):
            query_sum.forward(i)
    drain_t()
    drain_b()
    drain(("P3", "P4"))
    out_sum.drain()
    query_sum.drain()


def local(
    reps,
    shards,
    teacher_states,
    student_states,
    teacher_gain,
    student_gain,
    teacher_query,
    teacher_key,
    teacher_value,
    teacher_output,
    student_query,
    student_key,
    student_value,
    student_output,
    projection,
):
    length, d_t = teacher_states.shape
    rows, heads_s = student_query.shape
    d_s = rows * reps
    local_heads = heads_s // HD
    group_size = HQ_S // KV_S
    kv_width = max(local_heads // group_size, 1) * HD

    def kv_start_of(z):
        return lax.div(z * local_heads, group_size) * HD

    cosine, sine = tables(length)
    heads_t = teacher_query.shape[1]
    kv_t = teacher_key.shape[1]
    block_width = projection.shape[1]
    wide_s = 128
    wide_t = tile_of(block_width)
    count_s = d_s // wide_s
    per_block = block_width // wide_t
    most = (shards - 1) * per_block
    chips = reps // 2
    messages = 4 * (chips // 2) + 1
    ring_messages = 1 + 2 * (chips // 2 - 1)
    any_spec = pl.BlockSpec(memory_space=pl.ANY)
    vmem_spec = pl.BlockSpec(memory_space=pltpu.VMEM)
    sds = jax.ShapeDtypeStruct
    dma = pltpu.SemaphoreType.DMA

    def vmem(*shape, dtype=BF16):
        return pltpu.VMEM(shape, dtype)

    _, query_grad, output_grad = pl.pallas_call(
        partial(step_kernel, (reps, shards, kv_start_of)),
        out_shape=(
            sds((d_s, block_width), BF16),
            sds((rows, heads_s), F32),
            sds((rows, heads_s), F32),
        ),
        in_specs=[any_spec] * 2 + [vmem_spec] * 4 + [any_spec] * 9,
        out_specs=(any_spec, vmem_spec, vmem_spec),
        scratch_shapes=[
            vmem(d_s, heads_s),
            vmem(d_s, kv_width),
            vmem(d_s, kv_width),
            vmem(d_s, heads_s),
            vmem(d_t, heads_t),
            vmem(d_t, kv_t),
            vmem(d_t, kv_t),
            vmem(d_t, heads_t),
            vmem(length, d_s),
            vmem(length, d_t),
            vmem(length, d_s),
            vmem(count_s, length, wide_s),
            vmem(count_s, length, wide_s),
            vmem(count_s, length, wide_s),
            vmem(length, heads_s),
            vmem(length, kv_width),
            vmem(length, kv_width),
            vmem(length, heads_s),
            vmem(length, heads_t),
            vmem(length, kv_t),
            vmem(length, kv_t),
            vmem(length, heads_t),
            vmem(per_block, length, wide_t, dtype=F32),
            vmem(most, length, wide_t),
            vmem(most, length, wide_t),
            vmem(length, heads_s, dtype=F32),
            vmem(2, ring_messages, rows // 2, heads_s),
            vmem(2, ring_messages, rows // 2, heads_s),
            dma((9, messages)),
            dma((9, messages)),
            dma((9,)),
            dma((2, count_s)),
            dma((2, count_s)),
            dma((2, count_s)),
            dma((2, count_s)),
            dma((2, most)),
            dma((2, most)),
            dma((2, chips)),
            dma((2, chips)),
            dma((2, 2, ring_messages)),
            dma((2, 2, ring_messages)),
            dma((4,)),
            dma((2 + length // wide_s,)),
        ],
        compiler_params=pltpu.CompilerParams(
            collective_id=0, has_side_effects=True, vmem_limit_bytes=VMEM_BYTES
        ),
    )(
        student_states,
        teacher_states,
        student_gain.reshape(1, -1),
        teacher_gain.reshape(1, -1),
        jnp.asarray(cosine),
        jnp.asarray(sine),
        student_query,
        student_key,
        student_value,
        student_output,
        teacher_query,
        teacher_key,
        teacher_value,
        teacher_output,
        projection,
    )
    return (query_grad, output_grad)


def solution(mesh):
    return jax.shard_map(
        partial(local, mesh.shape["rep"], mesh.shape["shard"]),
        mesh=mesh,
        in_specs=(
            P("rep", None),
            P("rep", None),
            P(),
            P(),
            P("rep", "shard"),
            P("rep", "shard"),
            P("rep", "shard"),
            P("rep", "shard"),
            P("rep", "shard"),
            P("rep", None),
            P("rep", None),
            P("rep", "shard"),
            P("rep", "shard"),
        ),
        out_specs=(P("rep", "shard"), P("rep", "shard")),
        check_vma=False,
    )
```

```python
from functools import partial
import math

import jax
import jax.numpy as jnp
import numpy as np
from jax import lax
from jax.experimental import pallas as pl
from jax.experimental.pallas import tpu as pltpu
from jax.sharding import PartitionSpec as P

HQ_S = 16
KV_S = 4
HD = 128

theta_base = 1000000.0
norm_epsilon = 1e-06

F32 = jnp.float32
BF16 = jnp.bfloat16
VMEM_BYTES = 67_000_000
LAG = 2
AT = {"P1": 4, "P2a": 8, "P2b": 18, "P2a far": 21, "P2b far": 26, "P3": 32, "P4": 10, "P4 far": 13}


def tables(length):
    halfway = HD // 2
    inverse = theta_base ** (-(np.arange(halfway) * 2.0 / HD))
    inverse = inverse.astype(np.float32)
    angles = np.arange(length, dtype=np.float32)[:, None] * inverse[None, :]
    cosine = np.cos(angles)
    sine = np.sin(angles)
    return (
        np.concatenate([cosine, cosine], axis=1).astype(np.float32),
        np.concatenate([-sine, sine], axis=1).astype(np.float32),
    )


def tile_of(width):
    return 256 if width % 256 == 0 else 128


def dot_nt(left, right):
    return lax.dot_general(left, right, (((1,), (1,)), ((), ())), preferred_element_type=F32)


def dot_tn(left, right):
    return lax.dot_general(left, right, (((0,), (0,)), ((), ())), preferred_element_type=F32)


def span(index, size):
    return pl.ds(pl.multiple_of(index * size, size), size)


class Place:
    def __init__(self, reps, shards):
        self.reps = reps
        self.shards = shards
        self.chips = reps // 2
        self.r = lax.axis_index("rep")
        self.z = lax.axis_index("shard")
        chip = lax.div(self.r, 2)
        self.core = lax.rem(self.r, 2)
        row = lax.div(chip, 2)
        self.pos = 2 * row + lax.rem(lax.rem(chip, 2) + row, 2)
        self.partner = 2 * chip + 1 - self.core
        self.right = self.rep_at(1, self.core)
        self.left = self.rep_at(-1, self.core)

    def rep_at(self, step, core):
        place = lax.rem(self.pos + step + self.chips, self.chips)
        row = lax.div(place, 2)
        chip = 2 * row + lax.rem(lax.rem(place, 2) + row, 2)
        return 2 * chip + core

    def barrier(self, ring, line):
        sem = pltpu.get_barrier_semaphore()
        if ring:
            for target in (self.partner, self.left, self.right):
                pl.semaphore_signal(sem, inc=1, device_id={"rep": target})
        if line:

            @pl.when(self.z > 0)
            def _():
                pl.semaphore_signal(sem, inc=1, device_id={"shard": self.z - 1})

            @pl.when(self.z < self.shards - 1)
            def _():
                pl.semaphore_signal(sem, inc=1, device_id={"shard": self.z + 1})

        peers = 3 if ring else 0
        if line:
            peers += jnp.minimum(self.z, 1) + jnp.minimum(self.shards - 1 - self.z, 1)
        pl.semaphore_wait(sem, peers)


class Gather:
    def __init__(self, place, source, full, index, send_sem, recv_sem, local_sem):
        self.place = place
        self.source = source
        self.full = full
        self.index = index
        self.send_sem = send_sem
        self.recv_sem = recv_sem
        self.local_sem = local_sem
        self.rows = source.shape[0]
        self.half = place.chips // 2

    def slab(self, owner, part):
        if part is None:
            return self.full.at[pl.ds(pl.multiple_of(owner * self.rows, self.rows), self.rows)]
        rows = self.rows // 2
        return self.full.at[pl.ds(pl.multiple_of((2 * owner + part) * rows, rows), rows)]

    def copy(self, message, target, owner, part, source=None):
        slab = self.slab(owner, part)
        return pltpu.make_async_remote_copy(
            src_ref=slab if source is None else source,
            dst_ref=slab,
            send_sem=self.send_sem.at[self.index, message],
            recv_sem=self.recv_sem.at[self.index, message],
            device_id={"rep": target},
        )

    def part_of(self, step, way):
        return None if step < self.half else way

    def local(self):
        return pltpu.make_async_copy(
            self.source, self.slab(self.place.r, None), self.local_sem.at[self.index]
        )

    def start(self):
        p = self.place
        h = self.half
        self.copy(0, p.right, p.r, self.part_of(1, 0), self.source).start()
        self.copy(h, p.left, p.r, self.part_of(1, 1), self.source).start()
        self.copy(2 * h, p.partner, p.r, None, self.source).start()
        self.local().start()

    def relay(self, step):
        p = self.place
        h = self.half
        for way, sign, target in ((0, -1, p.right), (1, 1, p.left)):
            owner = p.rep_at(sign * step, p.core)
            base = way * h
            self.copy(base + step - 1, target, owner, self.part_of(step, way)).wait_recv()
            if step < h:
                self.copy(base + step, target, owner, self.part_of(step + 1, way)).start()
            self.copy(2 * h + base + step, p.partner, owner, self.part_of(step, way)).start()

    def finish(self, first, last):
        p = self.place
        h = self.half
        if first == 1:
            self.local().wait()
            self.copy(2 * h, p.partner, p.partner, None).wait_recv()
        for step in range(first, last + 1):
            for way, sign in ((0, -1), (1, 1)):
                owner = p.rep_at(sign * step, 1 - p.core)
                self.copy(
                    2 * h + way * h + step, p.partner, owner, self.part_of(step, way)
                ).wait_recv()

    def drain(self):
        p = self.place
        h = self.half
        for way, sign, target in ((0, -1, p.right), (1, 1, p.left)):
            for step in range(1, h + 1):
                owner = p.rep_at(sign * (step - 1), p.core)
                self.copy(way * h + step - 1, target, owner, self.part_of(step, way)).wait_send()
                owner = p.rep_at(sign * step, p.core)
                self.copy(
                    2 * h + way * h + step, p.partner, owner, self.part_of(step, way)
                ).wait_send()
        self.copy(2 * h, p.partner, p.r, None).wait_send()


def run_hooks(hooks, wave, last):
    for at, action in hooks:
        if at < last:
            pl.when(wave == at)(action)


def late_hooks(hooks, last):
    for at, action in hooks:
        if at >= last:
            action()


def line_sum(place, count, produce, consume, own, rightward, leftward, send_sem, recv_sem, hooks,
             done_hooks=()):
    z = place.z
    ends = place.shards - 1
    waves = count + LAG * ends

    def copy(way, j):
        buffer = (rightward, leftward)[way]
        return pltpu.make_async_remote_copy(
            src_ref=buffer.at[j],
            dst_ref=buffer.at[j],
            send_sem=send_sem.at[way, j],
            recv_sem=recv_sem.at[way, j],
            device_id={"shard": (z + 1, z - 1)[way]},
        )

    def has_before(way):
        return (z > 0, z < ends)[way]

    def has_after(way):
        return (z < ends, z > 0)[way]

    def valid(j):
        return (j >= 0) & (j < count)

    def wave_body(w, carry):
        at = (w - LAG * z, w - LAG * (ends - z))
        first = jnp.maximum(at[0], at[1])
        final = jnp.minimum(at[0], at[1])

        @pl.when(valid(first))
        def _():
            own[first] = produce(first).astype(BF16)

        for way in range(2):
            j = at[way]
            buffer = (rightward, leftward)[way]

            @pl.when(valid(j))
            def _():
                @pl.when(has_before(way))
                def _():
                    copy(way, j).wait_recv()
                    buffer[j] = (own[j].astype(F32) + buffer[j].astype(F32)).astype(BF16)

                @pl.when(jnp.logical_not(has_before(way)))
                def _():
                    buffer[j] = own[j]

                @pl.when(has_after(way))
                def _():
                    copy(way, j).start()

        @pl.when(valid(final))
        def _():
            total = rightward[final].astype(F32) + leftward[final].astype(F32)
            consume(final, total - own[final].astype(F32))
            run_hooks(done_hooks, final, count)

        run_hooks(hooks, w, waves)
        return carry

    lax.fori_loop(0, waves, wave_body, 0)
    late_hooks(hooks, waves)
    late_hooks(done_hooks, count)

    def drain(j, carry):
        for way in range(2):

            @pl.when(has_after(way))
            def _():
                copy(way, j).wait_send()

        return carry

    return lambda: lax.fori_loop(0, count, drain, 0)


def turn_of(u, late):
    return jnp.where((late == 0) & (u < 2), 1 - u, u)


def line_scatter(
    place, per_block, produce, own, late, rightward, leftward, send_sem, recv_sem, hooks
):
    z = place.z
    ends = place.shards - 1
    count = ends * per_block
    waves = count + LAG * ends

    def copy(way, q):
        buffer = (rightward, leftward)[way]
        return pltpu.make_async_remote_copy(
            src_ref=buffer.at[q],
            dst_ref=buffer.at[q],
            send_sem=send_sem.at[way, q],
            recv_sem=recv_sem.at[way, q],
            device_id={"shard": (z + 1, z - 1)[way]},
        )

    def block_at(way, q):
        last = late if way else ends - late
        return turn_of(lax.div(q, per_block), last)

    def wave_body(w, carry):
        for way in range(2):
            line = (z, ends - z)[way]
            q = w - LAG * line
            valid = (q >= 0) & (q < count)
            place_q = jnp.clip(q, 0, count - 1)
            block = block_at(way, place_q)
            chunk = lax.rem(place_q, per_block)
            buffer = (rightward, leftward)[way]
            before = line > 0

            @pl.when(valid & (block < ends - line))
            def _():
                target = (ends - block, block)[way]
                term = produce(target * per_block + chunk).astype(BF16)

                @pl.when(before)
                def _():
                    copy(way, q).wait_recv()
                    buffer[q] = (term.astype(F32) + buffer[q].astype(F32)).astype(BF16)

                @pl.when(jnp.logical_not(before))
                def _():
                    buffer[q] = term

                copy(way, q).start()

            @pl.when(valid & before & (block == ends - line))
            def _():
                copy(way, q).wait_recv()
                own[chunk] += buffer[q].astype(F32)

        run_hooks(hooks, w, waves)
        return carry

    lax.fori_loop(0, waves, wave_body, 0)
    late_hooks(hooks, waves)

    def finish():
        for way in range(2):
            line = (z, ends - z)[way]

            def drain(q, carry):
                @pl.when(block_at(way, q) < ends - line)
                def _():
                    copy(way, q).wait_send()

                return carry

            lax.fori_loop(0, count, drain, 0)

    return finish


class RingScatter:
    def __init__(self, place, partial_sums, pair, ring, out, index, pair_sems, ring_sems):
        self.place = place
        self.partial = partial_sums
        self.pair = pair
        self.ring = ring
        self.out = out
        self.index = index
        self.pair_sems = pair_sems
        self.ring_sems = ring_sems
        self.half = place.chips // 2
        self.rows = out.shape[0]
        self.steps = ring_order(place.chips)

    def exchange(self, i):
        self.pair_copy(i).start()

    def pair_copy(self, i):
        owner = self.place.rep_at(self.steps[i], 1 - self.place.core)
        return pltpu.make_async_remote_copy(
            src_ref=self.partial.at[span(owner, self.rows)],
            dst_ref=self.pair(i),
            send_sem=self.pair_sems[0].at[self.index, i],
            recv_sem=self.pair_sems[1].at[self.index, i],
            device_id={"rep": self.place.partner},
        )

    def message(self, step, part):
        return 0 if step == self.half else 1 + 2 * (self.half - 1 - step) + part

    def half_of(self, ref, part):
        return ref.at[pl.ds(part * (self.rows // 2), self.rows // 2)]

    def ring_copy(self, way, step, part, i):
        m = self.message(step, part)
        return pltpu.make_async_remote_copy(
            src_ref=self.half_of(self.pair(i), part),
            dst_ref=self.ring.at[way, m],
            send_sem=self.ring_sems[0].at[self.index, way, m],
            recv_sem=self.ring_sems[1].at[self.index, way, m],
            device_id={"rep": (self.place.right, self.place.left)[way]},
        )

    def moves(self, i):
        e, h = self.steps[i], self.half
        if e == h:
            return [(way, h, way, False) for way in range(2)]
        way, step = (0, e) if e > 0 else (1, -e)
        return [(way, step, part, part == way or step + 1 < h) for part in range(2)]

    def fresh(self, i, part):
        owner = self.place.rep_at(self.steps[i], self.place.core)
        rows = self.rows // 2
        mine = self.partial[span(2 * owner + part, rows), :].astype(F32)
        return mine + self.half_of(self.pair(i), part)[...].astype(F32)

    def incoming(self, way, step, part, i):
        self.ring_copy(way, step, part, i).wait_recv()
        return self.ring[way, self.message(step, part)].astype(F32)

    def forward(self, i):
        self.pair_copy(i).wait_recv()
        if self.steps[i] != 0:
            for way, step, part, has in self.moves(i):
                value = self.fresh(i, part)
                if has:
                    value = value + self.incoming(way, step + 1, part, i)
                self.half_of(self.pair(i), part)[...] = value.astype(BF16)
                self.ring_copy(way, step, part, i).start()
            return
        for part in range(2):
            value = self.fresh(i, part)
            for way in range(2):
                if part == way or self.half > 1:
                    value = value + self.incoming(way, 1, part, i)
            self.half_of(self.out, part)[...] = value

    def drain(self):
        for i, e in enumerate(self.steps):
            self.pair_copy(i).wait_send()
            if e != 0:
                for way, step, part, _ in self.moves(i):
                    self.ring_copy(way, step, part, i).wait_send()


def ring_order(chips):
    half = chips // 2
    order = [half]
    for step in range(half - 1, 0, -1):
        order += [step, -step]
    return order + [0]


def normalise(states, gain, block=16):
    length, width = states.shape

    def body(i, carry):
        at = pl.ds(pl.multiple_of(i * block, block), block)
        rows = states[at, :].astype(F32)
        meansq = jnp.sum(rows * rows, axis=-1, keepdims=True) * (1.0 / width)
        states[at, :] = (rows * lax.rsqrt(meansq + norm_epsilon) * gain[...][None, :]).astype(BF16)
        return carry

    lax.fori_loop(0, length // block, body, 0)


def turned(values, cosine, sine):
    return values * cosine + pltpu.roll(values, HD // 2, 1) * sine


def project(normed, weight, out, cosine, sine, first, count, tile):
    def body(t, carry):
        at = pl.ds(pl.multiple_of(t * tile, tile), tile)
        value = jnp.dot(normed[...], weight[:, at], preferred_element_type=F32)
        if cosine is None:
            out[:, at] = value.astype(BF16)
        else:
            for head in range(tile // HD):
                part = turned(value[:, head * HD : (head + 1) * HD], cosine[...], sine[...])
                spot = pl.ds(pl.multiple_of(t * tile + head * HD, HD), HD)
                out[:, spot] = part.astype(BF16)
        return carry

    lax.fori_loop(first, first + count, body, 0)


def soft(scores):
    highest = jnp.max(scores, axis=-1, keepdims=True)
    weights = jnp.exp(scores - highest)
    return weights / jnp.sum(weights, axis=-1, keepdims=True)


def masked_scores(query, keys):
    scores = dot_nt(query, keys) * HD ** (-0.5)
    row = lax.broadcasted_iota(jnp.int32, scores.shape, 0)
    column = lax.broadcasted_iota(jnp.int32, scores.shape, 1)
    return jnp.where(row >= column, scores, -1e30)


def attention(queries, keys, values, mixed, first, count, group):
    def body(h, carry):
        at = pl.ds(pl.multiple_of(h * HD, HD), HD)
        kv = pl.ds(pl.multiple_of(lax.div(h, group) * HD, HD), HD)
        probs = soft(masked_scores(queries[:, at], keys[:, kv])).astype(BF16)
        mixed[:, at] = jnp.dot(probs, values[:, kv], preferred_element_type=F32).astype(BF16)
        return carry

    lax.fori_loop(first, first + count, body, 0)


def backward_head(h, query, keys, values, grad_mixed, grad_query, cosine, sine, group):
    at = span(h, HD)
    kv = span(lax.div(h, group), HD)
    probs = soft(masked_scores(query[:, at], keys[:, kv]))
    grad_probs = dot_nt(grad_mixed[:, at].astype(BF16), values[:, kv]).astype(BF16).astype(F32)
    inner = jnp.sum(grad_probs * probs, axis=-1, keepdims=True)
    grad_scores = probs * (grad_probs - inner) * HD ** (-0.5)
    grad_rot = jnp.dot(grad_scores.astype(BF16), keys[:, kv], preferred_element_type=F32)
    grad_rot = grad_rot.astype(BF16).astype(F32)
    grad_query[:, at] = turned(grad_rot, cosine[...], -sine[...]).astype(BF16)


def step_kernel(
    sizes,
    states_s,
    states_t,
    gain_s,
    gain_t,
    cosine,
    sine,
    w_sq,
    w_sk,
    w_sv,
    w_so,
    w_tq,
    w_tk,
    w_tv,
    w_to,
    w_pj,
    map_full,
    query_grad,
    output_grad,
    sq,
    sk,
    sv,
    so,
    tq,
    tk,
    tv,
    to,
    normed_s,
    normed_t,
    hidden,
    own_s,
    right_s,
    left_s,
    query_s,
    key_s,
    value_s,
    mixed_s,
    query_t,
    key_t,
    value_t,
    mixed_t,
    attn_t,
    right_t,
    left_t,
    grad_mixed,
    ring_out,
    ring_query,
    gather_send,
    gather_recv,
    gather_local,
    sum_send,
    sum_recv,
    back_send,
    back_recv,
    scatter_send,
    scatter_recv,
    pair_send,
    pair_recv,
    ring_send,
    ring_recv,
    copies,
    map_sems,
):
    reps, shards, kv_start_of = sizes
    place = Place(reps, shards)
    length = normed_s.shape[0]
    kv_width = sk.shape[1]
    kv_at = pl.ds(pl.multiple_of(kv_start_of(place.z), HD), kv_width)
    sources = (w_sq, w_sk.at[:, kv_at], w_sv.at[:, kv_at], w_so, w_tq, w_tk, w_tv, w_to, w_pj)
    fulls = (sq, sk, sv, so, tq, tk, tv, to, map_full)
    weights = [
        Gather(place, source, full, i, gather_send, gather_recv, gather_local)
        for i, (source, full) in enumerate(zip(sources, fulls))
    ]
    half = place.chips // 2
    groups = {
        "P0": weights[0:3],
        "P1": weights[3:4],
        "P2a": weights[5:7],
        "P2b": weights[4:5],
        "P3": weights[7:8],
        "P4": weights[8:9],
    }

    def start(name):
        for weight in groups[name]:
            weight.start()

    def relay(name, step):
        for weight in groups[name]:
            weight.relay(step)

    def near(name):
        for step in range(2, half):
            relay(name, step)
        for weight in groups[name]:
            weight.finish(1, half - 1)

    def far(name):
        relay(name, half)
        for weight in groups[name]:
            weight.finish(half, half)

    def finish(name):
        near(name)
        far(name)

    def drain(names):
        for name in names:
            for weight in groups[name]:
                weight.drain()

    in_s = pltpu.make_async_copy(states_s, normed_s, copies.at[0])
    in_h = pltpu.make_async_copy(states_s, hidden, copies.at[1])
    in_t = pltpu.make_async_copy(states_t, normed_t, copies.at[2])
    in_s.start()
    place.barrier(True, True)
    start("P0")
    in_h.start()
    in_t.start()
    in_s.wait()
    normalise(normed_s, gain_s)
    relay("P0", 1)
    start("P1")
    in_t.wait()
    normalise(normed_t, gain_t)
    finish("P0")
    tile = tile_of(sq.shape[1])
    kv_tile = tile_of(kv_width)
    project(normed_s, sk, key_s, cosine, sine, 0, kv_width // kv_tile, kv_tile)
    project(normed_s, sv, value_s, None, None, 0, kv_width // kv_tile, kv_tile)
    project(normed_s, sq, query_s, cosine, sine, 0, sq.shape[1] // tile, tile)
    relay("P1", 1)
    start("P2a")
    start("P2b")
    heads = sq.shape[1] // HD
    group = heads // (kv_width // HD)
    attention(query_s, key_s, value_s, mixed_s, 0, heads, group)
    near("P1")
    in_h.wait()

    count, _, width = own_s.shape
    block_width = map_full.shape[1]
    states_at = pl.ds(pl.multiple_of(place.z * block_width, 128), block_width)
    in_b = pltpu.make_async_copy(
        states_t.at[:, states_at], normed_t.at[:, 0:block_width], copies.at[3]
    )

    steps = ring_order(place.chips)
    per_chip = count // place.chips
    in_order = per_chip * place.chips == count
    if not in_order:
        far("P1")

    def tile_at(j, order):
        if not in_order:
            return j
        turn = lax.div(j, per_chip)
        chip = 0
        for i, step in enumerate(order):
            chip = chip + jnp.where(turn == i, lax.div(place.rep_at(step, 0), 2), 0)
        return chip * per_chip + lax.rem(j, per_chip)

    def produce_s(j):
        return dot_nt(mixed_s[...], so[span(tile_at(j, steps[::-1]), width), :])

    def consume_s(j, total):
        at = span(tile_at(j, steps[::-1]), width)
        hidden[:, at] = (hidden[:, at].astype(F32) + total).astype(BF16)

    t_tile = tile_of(tq.shape[1])
    t_kv = tile_of(tk.shape[1])
    t_heads = tq.shape[1] // HD
    t_group = t_heads // (tk.shape[1] // HD)
    hooks = [(AT["P1"], lambda: far("P1"))] if in_order else []
    hooks += [
        (AT["P2a"], lambda: relay("P2a", 1)),
        (AT["P2b"], lambda: relay("P2b", 1)),
        (AT["P2b"], lambda: start("P3")),
        (AT["P2a far"], lambda: finish("P2a")),
        (AT["P2b far"], lambda: finish("P2b")),
    ]
    tasks = []
    for t in range(tk.shape[1] // t_kv):
        tasks.append(partial(project, normed_t, tk, key_t, cosine, sine, t, 1, t_kv))
        tasks.append(partial(project, normed_t, tv, value_t, None, None, t, 1, t_kv))
    for t in range(tq.shape[1] // t_tile):
        tasks.append(partial(project, normed_t, tq, query_t, cosine, sine, t, 1, t_tile))
    tasks.append(lambda: drain(("P0", "P1", "P2a", "P2b")))
    tasks.append(in_b.start)
    for h in range(t_heads):
        tasks.append(partial(attention, query_t, key_t, value_t, mixed_t, h, 1, t_group))
    hooks += [(AT["P2b far"] + i // 2, task) for i, task in enumerate(tasks)]
    hooks.append((AT["P3"], lambda: relay("P3", 1)))
    hooks.append((AT["P3"], lambda: start("P4")))
    drain_s = line_sum(
        place, count, produce_s, consume_s, own_s, right_s, left_s, sum_send, sum_recv, hooks
    )
    drain_s()
    near("P3")
    by_chip = shards == place.chips
    if not by_chip:
        far("P3")

    per_block, _, width_t = attn_t.shape
    in_b.wait()

    def produce_t(j):
        return dot_nt(mixed_t[...], to[span(j, width_t), :])

    columns = (tk, tv)

    def column_copy(t):
        return pltpu.make_async_copy(
            map_full.at[:, t * width_t : (t + 1) * width_t],
            columns[t % 2].at[0 : map_full.shape[0]],
            map_sems.at[t % 2],
        )

    def first_columns():
        for t in range(min(2, per_block)):
            column_copy(t).start()

    def predict(t):
        column_copy(t).wait()
        product = jnp.dot(
            hidden[...], columns[t % 2][0 : map_full.shape[0]], preferred_element_type=F32
        )
        at = pl.ds(t * width_t, width_t)
        attn_t[t] += normed_t[:, at].astype(F32) - product
        if t + 2 < per_block:
            column_copy(t + 2).start()

    def own_terms():
        for t in range(per_block):
            attn_t[t] += produce_t(place.z * per_block + t).astype(BF16).astype(F32)

    attn_t[...] = jnp.zeros_like(attn_t)
    hooks = [(per_block - 1, lambda: far("P3"))] if by_chip else []
    hooks += [(per_block, own_terms), (AT["P4"], lambda: relay("P4", 1))]
    hooks += [(AT["P4 far"], lambda: finish("P4")), (AT["P4 far"], first_columns)]
    hooks += [(AT["P4 far"] + 1 + t, partial(predict, t)) for t in range(per_block)]
    opposite = lax.div(place.rep_at(half, 0), 2)
    drain_t = line_scatter(
        place, per_block, produce_t, attn_t, opposite if by_chip else place.shards - 1, right_t,
        left_t, scatter_send, scatter_recv, hooks,
    )
    scaling = 1.0 / math.sqrt(reps * length)
    grad_pred = normed_t.at[:, 0:block_width]
    for t in range(per_block):
        grad_pred[:, t * width_t : (t + 1) * width_t] = (attn_t[t] * -scaling).astype(BF16)

    rows = query_grad.shape[0]
    wide = query_grad.shape[1]
    pair_sems = (pair_send, pair_recv)
    ring_sems = (ring_send, ring_recv)

    def slot(first):
        return lambda i: tq.at[(first + i) * rows : (first + i + 1) * rows, 0:wide]

    out_sum = RingScatter(
        place, sq, slot(0), ring_out, output_grad, 0, pair_sems, ring_sems
    )
    query_sum = RingScatter(
        place, so, slot(place.chips), ring_query, query_grad, 1, pair_sems, ring_sems
    )
    slots = length // width

    def rows_copy(j):
        slot_at = lax.rem(j, slots)
        return pltpu.make_async_copy(
            map_full.at[span(tile_at(j, steps), width)],
            normed_t.at[span(slot_at, width), block_width : 2 * block_width],
            map_sems.at[2 + slot_at],
        )

    def produce_b(j):
        rows_copy(j).wait()
        at = span(lax.rem(j, slots), width)
        product = dot_nt(grad_pred[...], normed_t[at, block_width : 2 * block_width])

        @pl.when(j + slots < count)
        def _():
            rows_copy(j + slots).start()

        return product

    grad_mixed[...] = jnp.zeros_like(grad_mixed)

    def consume_b(j, total):
        at = span(tile_at(j, steps), width)
        grad = total.astype(BF16)
        grad_mixed[...] += jnp.dot(grad, so[at, :], preferred_element_type=F32)
        sq[at, :] = dot_tn(grad, mixed_s[...]).astype(BF16)

    for j in range(min(slots, count)):
        rows_copy(j).start()
    done = []
    for i in range(place.chips):
        ready = (i + 1) * per_chip - 1 if in_order else count
        done.append((ready, partial(out_sum.exchange, i)))
        done.append((ready + 3 if in_order else count, partial(out_sum.forward, i)))
    drain_b = line_sum(
        place, count, produce_b, consume_b, own_s, right_s, left_s, back_send, back_recv, [], done
    )
    grad_query = query_t.at[:, 0:wide]

    def one_head(h, carry):
        backward_head(h, query_s, key_s, value_s, grad_mixed, grad_query, cosine, sine, group)
        return carry

    lax.fori_loop(0, heads, one_head, 0)

    def query_tile(t, carry):
        so[span(t, width), :] = dot_tn(normed_s[:, span(t, width)], grad_query[...]).astype(BF16)
        return carry

    if in_order:
        for i, step in enumerate(steps):
            first = lax.div(place.rep_at(step, 0), 2) * per_chip
            lax.fori_loop(first, first + per_chip, query_tile, 0)
            query_sum.exchange(i)
            if i > 0:
                query_sum.forward(i - 1)
        query_sum.forward(len(steps) - 1)
    else:
        lax.fori_loop(0, count, query_tile, 0)
        for i in range(len(steps)):
            query_sum.exchange(i)
        for i in range(len(steps)):
            query_sum.forward(i)
    drain_t()
    drain_b()
    drain(("P3", "P4"))
    out_sum.drain()
    query_sum.drain()


def local(
    reps,
    shards,
    teacher_states,
    student_states,
    teacher_gain,
    student_gain,
    teacher_query,
    teacher_key,
    teacher_value,
    teacher_output,
    student_query,
    student_key,
    student_value,
    student_output,
    projection,
):
    length, d_t = teacher_states.shape
    rows, heads_s = student_query.shape
    d_s = rows * reps
    local_heads = heads_s // HD
    group_size = HQ_S // KV_S
    kv_width = max(local_heads // group_size, 1) * HD

    def kv_start_of(z):
        return lax.div(z * local_heads, group_size) * HD

    cosine, sine = tables(length)
    heads_t = teacher_query.shape[1]
    kv_t = teacher_key.shape[1]
    block_width = projection.shape[1]
    wide_s = 128
    wide_t = tile_of(block_width)
    count_s = d_s // wide_s
    per_block = block_width // wide_t
    most = (shards - 1) * per_block
    chips = reps // 2
    messages = 4 * (chips // 2) + 1
    ring_messages = 1 + 2 * (chips // 2 - 1)
    any_spec = pl.BlockSpec(memory_space=pl.ANY)
    vmem_spec = pl.BlockSpec(memory_space=pltpu.VMEM)
    sds = jax.ShapeDtypeStruct
    dma = pltpu.SemaphoreType.DMA

    def vmem(*shape, dtype=BF16):
        return pltpu.VMEM(shape, dtype)

    _, query_grad, output_grad = pl.pallas_call(
        partial(step_kernel, (reps, shards, kv_start_of)),
        out_shape=(
            sds((d_s, block_width), BF16),
            sds((rows, heads_s), F32),
            sds((rows, heads_s), F32),
        ),
        in_specs=[any_spec] * 2 + [vmem_spec] * 4 + [any_spec] * 9,
        out_specs=(any_spec, vmem_spec, vmem_spec),
        scratch_shapes=[
            vmem(d_s, heads_s),
            vmem(d_s, kv_width),
            vmem(d_s, kv_width),
            vmem(d_s, heads_s),
            vmem(d_t, heads_t),
            vmem(d_t, kv_t),
            vmem(d_t, kv_t),
            vmem(d_t, heads_t),
            vmem(length, d_s),
            vmem(length, d_t),
            vmem(length, d_s),
            vmem(count_s, length, wide_s),
            vmem(count_s, length, wide_s),
            vmem(count_s, length, wide_s),
            vmem(length, heads_s),
            vmem(length, kv_width),
            vmem(length, kv_width),
            vmem(length, heads_s),
            vmem(length, heads_t),
            vmem(length, kv_t),
            vmem(length, kv_t),
            vmem(length, heads_t),
            vmem(per_block, length, wide_t, dtype=F32),
            vmem(most, length, wide_t),
            vmem(most, length, wide_t),
            vmem(length, heads_s, dtype=F32),
            vmem(2, ring_messages, rows // 2, heads_s),
            vmem(2, ring_messages, rows // 2, heads_s),
            dma((9, messages)),
            dma((9, messages)),
            dma((9,)),
            dma((2, count_s)),
            dma((2, count_s)),
            dma((2, count_s)),
            dma((2, count_s)),
            dma((2, most)),
            dma((2, most)),
            dma((2, chips)),
            dma((2, chips)),
            dma((2, 2, ring_messages)),
            dma((2, 2, ring_messages)),
            dma((4,)),
            dma((2 + length // wide_s,)),
        ],
        compiler_params=pltpu.CompilerParams(
            collective_id=0, has_side_effects=True, vmem_limit_bytes=VMEM_BYTES
        ),
    )(
        student_states,
        teacher_states,
        student_gain,
        teacher_gain,
        jnp.asarray(cosine),
        jnp.asarray(sine),
        student_query,
        student_key,
        student_value,
        student_output,
        teacher_query,
        teacher_key,
        teacher_value,
        teacher_output,
        projection,
    )
    return (query_grad, output_grad)


def solution(mesh):
    return jax.shard_map(
        partial(local, mesh.shape["rep"], mesh.shape["shard"]),
        mesh=mesh,
        in_specs=(
            P("rep", None),
            P("rep", None),
            P(),
            P(),
            P("rep", "shard"),
            P("rep", "shard"),
            P("rep", "shard"),
            P("rep", "shard"),
            P("rep", "shard"),
            P("rep", None),
            P("rep", None),
            P("rep", "shard"),
            P("rep", "shard"),
        ),
        out_specs=(P("rep", "shard"), P("rep", "shard")),
        check_vma=False,
    )
```

```python
from functools import partial
import math

import jax
import jax.numpy as jnp
import numpy as np
from jax import lax
from jax.experimental import pallas as pl
from jax.experimental.pallas import tpu as pltpu
from jax.sharding import PartitionSpec as P

HQ_S = 16
KV_S = 4
HD = 128

theta_base = 1000000.0
norm_epsilon = 1e-06

F32 = jnp.float32
BF16 = jnp.bfloat16
VMEM_BYTES = 67_000_000
LAG = 2
AT = {"P1": 10, "P2a": 8, "P2b": 18, "P2b near": 20, "P2a far": 24, "P2b far": 26, "P3": 40, "P4": 9, "P4 far": 14}


def tables(length):
    halfway = HD // 2
    inverse = theta_base ** (-(np.arange(halfway) * 2.0 / HD))
    inverse = inverse.astype(np.float32)
    angles = np.arange(length, dtype=np.float32)[:, None] * inverse[None, :]
    cosine = np.cos(angles)
    sine = np.sin(angles)
    return (
        np.concatenate([cosine, cosine], axis=1).astype(np.float32),
        np.concatenate([-sine, sine], axis=1).astype(np.float32),
    )


def tile_of(width):
    return 256 if width % 256 == 0 else 128


def dot_nt(left, right):
    return lax.dot_general(left, right, (((1,), (1,)), ((), ())), preferred_element_type=F32)


def dot_tn(left, right):
    return lax.dot_general(left, right, (((0,), (0,)), ((), ())), preferred_element_type=F32)


def span(index, size):
    return pl.ds(pl.multiple_of(index * size, size), size)


class Place:
    def __init__(self, reps, shards):
        self.reps = reps
        self.shards = shards
        self.chips = reps // 2
        self.r = lax.axis_index("rep")
        self.z = lax.axis_index("shard")
        chip = lax.div(self.r, 2)
        self.core = lax.rem(self.r, 2)
        row = lax.div(chip, 2)
        self.pos = 2 * row + lax.rem(lax.rem(chip, 2) + row, 2)
        self.partner = 2 * chip + 1 - self.core
        self.right = self.rep_at(1, self.core)
        self.left = self.rep_at(-1, self.core)

    def rep_at(self, step, core):
        place = lax.rem(self.pos + step + self.chips, self.chips)
        row = lax.div(place, 2)
        chip = 2 * row + lax.rem(lax.rem(place, 2) + row, 2)
        return 2 * chip + core

    def barrier(self, ring, line):
        sem = pltpu.get_barrier_semaphore()
        if ring:
            for target in (self.partner, self.left, self.right):
                pl.semaphore_signal(sem, inc=1, device_id={"rep": target})
        if line:

            @pl.when(self.z > 0)
            def _():
                pl.semaphore_signal(sem, inc=1, device_id={"shard": self.z - 1})

            @pl.when(self.z < self.shards - 1)
            def _():
                pl.semaphore_signal(sem, inc=1, device_id={"shard": self.z + 1})

        peers = 3 if ring else 0
        if line:
            peers += jnp.minimum(self.z, 1) + jnp.minimum(self.shards - 1 - self.z, 1)
        pl.semaphore_wait(sem, peers)


class Gather:
    def __init__(self, place, source, full, index, send_sem, recv_sem, local_sem):
        self.place = place
        self.source = source
        self.full = full
        self.index = index
        self.send_sem = send_sem
        self.recv_sem = recv_sem
        self.local_sem = local_sem
        self.rows = source.shape[0]
        self.half = place.chips // 2

    def slab(self, owner, part):
        if part is None:
            return self.full.at[pl.ds(pl.multiple_of(owner * self.rows, self.rows), self.rows)]
        rows = self.rows // 2
        return self.full.at[pl.ds(pl.multiple_of((2 * owner + part) * rows, rows), rows)]

    def copy(self, message, target, owner, part, source=None):
        slab = self.slab(owner, part)
        return pltpu.make_async_remote_copy(
            src_ref=slab if source is None else source,
            dst_ref=slab,
            send_sem=self.send_sem.at[self.index, message],
            recv_sem=self.recv_sem.at[self.index, message],
            device_id={"rep": target},
        )

    def part_of(self, step, way):
        return None if step < self.half else way

    def local(self):
        return pltpu.make_async_copy(
            self.source, self.slab(self.place.r, None), self.local_sem.at[self.index]
        )

    def start(self):
        p = self.place
        h = self.half
        self.copy(0, p.right, p.r, self.part_of(1, 0), self.source).start()
        self.copy(h, p.left, p.r, self.part_of(1, 1), self.source).start()
        self.copy(2 * h, p.partner, p.r, None, self.source).start()
        self.local().start()

    def relay(self, step):
        p = self.place
        h = self.half
        for way, sign, target in ((0, -1, p.right), (1, 1, p.left)):
            owner = p.rep_at(sign * step, p.core)
            base = way * h
            self.copy(base + step - 1, target, owner, self.part_of(step, way)).wait_recv()
            if step < h:
                self.copy(base + step, target, owner, self.part_of(step + 1, way)).start()
            self.copy(2 * h + base + step, p.partner, owner, self.part_of(step, way)).start()

    def finish(self, first, last):
        p = self.place
        h = self.half
        if first == 1:
            self.local().wait()
            self.copy(2 * h, p.partner, p.partner, None).wait_recv()
        for step in range(first, last + 1):
            for way, sign in ((0, -1), (1, 1)):
                owner = p.rep_at(sign * step, 1 - p.core)
                self.copy(
                    2 * h + way * h + step, p.partner, owner, self.part_of(step, way)
                ).wait_recv()

    def drain(self):
        p = self.place
        h = self.half
        for way, sign, target in ((0, -1, p.right), (1, 1, p.left)):
            for step in range(1, h + 1):
                owner = p.rep_at(sign * (step - 1), p.core)
                self.copy(way * h + step - 1, target, owner, self.part_of(step, way)).wait_send()
                owner = p.rep_at(sign * step, p.core)
                self.copy(
                    2 * h + way * h + step, p.partner, owner, self.part_of(step, way)
                ).wait_send()
        self.copy(2 * h, p.partner, p.r, None).wait_send()


def run_hooks(hooks, wave, last):
    for at, action in hooks:
        if at < last:
            pl.when(wave == at)(action)


def late_hooks(hooks, last):
    for at, action in hooks:
        if at >= last:
            action()


def line_sum(place, count, produce, consume, own, rightward, leftward, send_sem, recv_sem, hooks,
             done_hooks=()):
    z = place.z
    ends = place.shards - 1
    waves = count + LAG * ends

    def copy(way, j):
        buffer = (rightward, leftward)[way]
        return pltpu.make_async_remote_copy(
            src_ref=buffer.at[j],
            dst_ref=buffer.at[j],
            send_sem=send_sem.at[way, j],
            recv_sem=recv_sem.at[way, j],
            device_id={"shard": (z + 1, z - 1)[way]},
        )

    def has_before(way):
        return (z > 0, z < ends)[way]

    def has_after(way):
        return (z < ends, z > 0)[way]

    def valid(j):
        return (j >= 0) & (j < count)

    def wave_body(w, carry):
        at = (w - LAG * z, w - LAG * (ends - z))
        first = jnp.maximum(at[0], at[1])
        final = jnp.minimum(at[0], at[1])

        @pl.when(valid(first))
        def _():
            own[first] = produce(first).astype(BF16)

        for way in range(2):
            j = at[way]
            buffer = (rightward, leftward)[way]

            @pl.when(valid(j))
            def _():
                @pl.when(has_before(way))
                def _():
                    copy(way, j).wait_recv()
                    buffer[j] = (own[j].astype(F32) + buffer[j].astype(F32)).astype(BF16)

                @pl.when(jnp.logical_not(has_before(way)))
                def _():
                    buffer[j] = own[j]

                @pl.when(has_after(way))
                def _():
                    copy(way, j).start()

        @pl.when(valid(final))
        def _():
            total = rightward[final].astype(F32) + leftward[final].astype(F32)
            consume(final, total - own[final].astype(F32))
            run_hooks(done_hooks, final, count)

        run_hooks(hooks, w, waves)
        return carry

    lax.fori_loop(0, waves, wave_body, 0)
    late_hooks(hooks, waves)
    late_hooks(done_hooks, count)

    def drain(j, carry):
        for way in range(2):

            @pl.when(has_after(way))
            def _():
                copy(way, j).wait_send()

        return carry

    return lambda: lax.fori_loop(0, count, drain, 0)


def turn_of(u, late):
    return jnp.where((late == 0) & (u < 2), 1 - u, u)


def line_scatter(
    place, per_block, produce, own, late, rightward, leftward, send_sem, recv_sem, hooks
):
    z = place.z
    ends = place.shards - 1
    count = ends * per_block
    waves = count + LAG * ends

    def copy(way, q):
        buffer = (rightward, leftward)[way]
        return pltpu.make_async_remote_copy(
            src_ref=buffer.at[q],
            dst_ref=buffer.at[q],
            send_sem=send_sem.at[way, q],
            recv_sem=recv_sem.at[way, q],
            device_id={"shard": (z + 1, z - 1)[way]},
        )

    def block_at(way, q):
        last = late if way else ends - late
        return turn_of(lax.div(q, per_block), last)

    def wave_body(w, carry):
        for way in range(2):
            line = (z, ends - z)[way]
            q = w - LAG * line
            valid = (q >= 0) & (q < count)
            place_q = jnp.clip(q, 0, count - 1)
            block = block_at(way, place_q)
            chunk = lax.rem(place_q, per_block)
            buffer = (rightward, leftward)[way]
            before = line > 0

            @pl.when(valid & (block < ends - line))
            def _():
                target = (ends - block, block)[way]
                term = produce(target * per_block + chunk).astype(BF16)

                @pl.when(before)
                def _():
                    copy(way, q).wait_recv()
                    buffer[q] = (term.astype(F32) + buffer[q].astype(F32)).astype(BF16)

                @pl.when(jnp.logical_not(before))
                def _():
                    buffer[q] = term

                copy(way, q).start()

            @pl.when(valid & before & (block == ends - line))
            def _():
                copy(way, q).wait_recv()
                own[chunk] += buffer[q].astype(F32)

        run_hooks(hooks, w, waves)
        return carry

    lax.fori_loop(0, waves, wave_body, 0)
    late_hooks(hooks, waves)

    def finish():
        for way in range(2):
            line = (z, ends - z)[way]

            def drain(q, carry):
                @pl.when(block_at(way, q) < ends - line)
                def _():
                    copy(way, q).wait_send()

                return carry

            lax.fori_loop(0, count, drain, 0)

    return finish


class RingScatter:
    def __init__(self, place, partial_sums, pair, ring, out, index, pair_sems, ring_sems):
        self.place = place
        self.partial = partial_sums
        self.pair = pair
        self.ring = ring
        self.out = out
        self.index = index
        self.pair_sems = pair_sems
        self.ring_sems = ring_sems
        self.half = place.chips // 2
        self.rows = out.shape[0]
        self.steps = ring_order(place.chips)

    def exchange(self, i):
        self.pair_copy(i).start()

    def pair_copy(self, i):
        owner = self.place.rep_at(self.steps[i], 1 - self.place.core)
        return pltpu.make_async_remote_copy(
            src_ref=self.partial.at[span(owner, self.rows)],
            dst_ref=self.pair(i),
            send_sem=self.pair_sems[0].at[self.index, i],
            recv_sem=self.pair_sems[1].at[self.index, i],
            device_id={"rep": self.place.partner},
        )

    def message(self, step, part):
        return 0 if step == self.half else 1 + 2 * (self.half - 1 - step) + part

    def half_of(self, ref, part):
        return ref.at[pl.ds(part * (self.rows // 2), self.rows // 2)]

    def ring_copy(self, way, step, part, i):
        m = self.message(step, part)
        return pltpu.make_async_remote_copy(
            src_ref=self.half_of(self.pair(i), part),
            dst_ref=self.ring(way, m),
            send_sem=self.ring_sems[0].at[self.index, way, m],
            recv_sem=self.ring_sems[1].at[self.index, way, m],
            device_id={"rep": (self.place.right, self.place.left)[way]},
        )

    def moves(self, i):
        e, h = self.steps[i], self.half
        if e == h:
            return [(way, h, way, False) for way in range(2)]
        way, step = (0, e) if e > 0 else (1, -e)
        return [(way, step, part, part == way or step + 1 < h) for part in range(2)]

    def fresh(self, i, part):
        owner = self.place.rep_at(self.steps[i], self.place.core)
        rows = self.rows // 2
        mine = self.partial[span(2 * owner + part, rows), :].astype(F32)
        return mine + self.half_of(self.pair(i), part)[...].astype(F32)

    def incoming(self, way, step, part, i):
        self.ring_copy(way, step, part, i).wait_recv()
        return self.ring(way, self.message(step, part))[...].astype(F32)

    def send(self, i, summed):
        for way, step, part, has in self.moves(i):
            if has == summed:
                value = self.fresh(i, part)
                if has:
                    value = value + self.incoming(way, step + 1, part, i)
                self.half_of(self.pair(i), part)[...] = value.astype(BF16)
                self.ring_copy(way, step, part, i).start()

    def send_fresh(self, i):
        self.pair_copy(i).wait_recv()
        if self.steps[i] != 0:
            self.send(i, False)

    def send_sums(self, i):
        if self.steps[i] != 0:
            self.send(i, True)
            return
        for part in range(2):
            value = self.fresh(i, part)
            for way in range(2):
                if part == way or self.half > 1:
                    value = value + self.incoming(way, 1, part, i)
            self.half_of(self.out, part)[...] = value

    def forward(self, i):
        self.send_fresh(i)
        self.send_sums(i)

    def drain(self):
        for i, e in enumerate(self.steps):
            self.pair_copy(i).wait_send()
            if e != 0:
                for way, step, part, _ in self.moves(i):
                    self.ring_copy(way, step, part, i).wait_send()


def ring_order(chips):
    half = chips // 2
    order = [half]
    for step in range(half - 1, 0, -1):
        order += [step, -step]
    return order + [0]


def normalise(states, gain, block=16):
    length, width = states.shape

    def body(i, carry):
        at = pl.ds(pl.multiple_of(i * block, block), block)
        rows = states[at, :].astype(F32)
        meansq = jnp.sum(rows * rows, axis=-1, keepdims=True) * (1.0 / width)
        states[at, :] = (rows * lax.rsqrt(meansq + norm_epsilon) * gain[...][None, :]).astype(BF16)
        return carry

    lax.fori_loop(0, length // block, body, 0)


def turned(values, cosine, sine):
    return values * cosine + pltpu.roll(values, HD // 2, 1) * sine


def project(normed, weight, out, cosine, sine, first, count, tile):
    def body(t, carry):
        at = pl.ds(pl.multiple_of(t * tile, tile), tile)
        value = jnp.dot(normed[...], weight[:, at], preferred_element_type=F32)
        if cosine is None:
            out[:, at] = value.astype(BF16)
        else:
            for head in range(tile // HD):
                part = turned(value[:, head * HD : (head + 1) * HD], cosine[...], sine[...])
                spot = pl.ds(pl.multiple_of(t * tile + head * HD, HD), HD)
                out[:, spot] = part.astype(BF16)
        return carry

    lax.fori_loop(first, first + count, body, 0)


def project_near(place, normed, weight, total, t, tile):
    at = span(t, tile)
    size = weight.shape[0] // place.chips
    value = None
    for step in ring_order(place.chips)[1:]:
        rows = span(lax.div(place.rep_at(step, 0), 2), size)
        term = jnp.dot(normed[:, rows], weight[rows, at], preferred_element_type=F32)
        value = term if value is None else value + term
    total[...] = value


def project_far(place, normed, weight, total, out, cosine, sine, t, tile):
    at = span(t, tile)
    size = weight.shape[0] // place.chips
    rows = span(lax.div(place.rep_at(place.chips // 2, 0), 2), size)
    value = total[...] + jnp.dot(normed[:, rows], weight[rows, at], preferred_element_type=F32)
    if cosine is None:
        out[:, at] = value.astype(BF16)
    else:
        for head in range(tile // HD):
            part = turned(value[:, head * HD : (head + 1) * HD], cosine[...], sine[...])
            out[:, t * tile + head * HD : t * tile + (head + 1) * HD] = part.astype(BF16)


def soft(scores):
    highest = jnp.max(scores, axis=-1, keepdims=True)
    weights = jnp.exp(scores - highest)
    return weights / jnp.sum(weights, axis=-1, keepdims=True)


def masked_scores(query, keys):
    scores = dot_nt(query, keys) * HD ** (-0.5)
    row = lax.broadcasted_iota(jnp.int32, scores.shape, 0)
    column = lax.broadcasted_iota(jnp.int32, scores.shape, 1)
    return jnp.where(row >= column, scores, -1e30)


def attention(queries, keys, values, mixed, first, count, group):
    def body(h, carry):
        at = pl.ds(pl.multiple_of(h * HD, HD), HD)
        kv = pl.ds(pl.multiple_of(lax.div(h, group) * HD, HD), HD)
        probs = soft(masked_scores(queries[:, at], keys[:, kv])).astype(BF16)
        mixed[:, at] = jnp.dot(probs, values[:, kv], preferred_element_type=F32).astype(BF16)
        return carry

    lax.fori_loop(first, first + count, body, 0)


def backward_head(h, query, keys, values, grad_mixed, grad_query, cosine, sine, group):
    at = span(h, HD)
    kv = span(lax.div(h, group), HD)
    probs = soft(masked_scores(query[:, at], keys[:, kv]))
    grad_probs = dot_nt(grad_mixed[:, at].astype(BF16), values[:, kv]).astype(BF16).astype(F32)
    inner = jnp.sum(grad_probs * probs, axis=-1, keepdims=True)
    grad_scores = probs * (grad_probs - inner) * HD ** (-0.5)
    grad_rot = jnp.dot(grad_scores.astype(BF16), keys[:, kv], preferred_element_type=F32)
    grad_rot = grad_rot.astype(BF16).astype(F32)
    grad_query[:, at] = turned(grad_rot, cosine[...], -sine[...]).astype(BF16)


def step_kernel(
    sizes,
    states_s,
    states_t,
    gain_s,
    gain_t,
    cosine,
    sine,
    w_sq,
    w_sk,
    w_sv,
    w_so,
    w_tq,
    w_tk,
    w_tv,
    w_to,
    w_pj,
    map_full,
    query_grad,
    output_grad,
    sq,
    sk,
    sv,
    so,
    tq,
    tk,
    tv,
    to,
    normed_s,
    normed_t,
    hidden,
    own_s,
    right_s,
    left_s,
    query_s,
    key_s,
    value_s,
    mixed_s,
    query_t,
    key_t,
    value_t,
    mixed_t,
    attn_t,
    right_t,
    left_t,
    grad_mixed,
    ring_out,
    ring_query,
    query_total,
    out_total,
    gather_send,
    gather_recv,
    gather_local,
    sum_send,
    sum_recv,
    scatter_send,
    scatter_recv,
    pair_send,
    pair_recv,
    ring_send,
    ring_recv,
    copies,
    map_sems,
):
    reps, shards, kv_start_of = sizes
    place = Place(reps, shards)
    length = normed_s.shape[0]
    kv_width = sk.shape[1]
    kv_at = pl.ds(pl.multiple_of(kv_start_of(place.z), HD), kv_width)
    sources = (w_sq, w_sk.at[:, kv_at], w_sv.at[:, kv_at], w_so, w_tq, w_tk, w_tv, w_to, w_pj)
    fulls = (sq, sk, sv, so, tq, tk, tv, to, map_full)
    weights = [
        Gather(place, source, full, i, gather_send, gather_recv, gather_local)
        for i, (source, full) in enumerate(zip(sources, fulls))
    ]
    half = place.chips // 2
    groups = {
        "P0": weights[0:3],
        "P1": weights[3:4],
        "P2a": weights[5:7],
        "P2b": weights[4:5],
        "P3": weights[7:8],
        "P4": weights[8:9],
    }

    def start(name):
        for weight in groups[name]:
            weight.start()

    def relay(name, step):
        for weight in groups[name]:
            weight.relay(step)

    def near(name):
        for step in range(2, half):
            relay(name, step)
        for weight in groups[name]:
            weight.finish(1, half - 1)

    def far(name):
        relay(name, half)
        for weight in groups[name]:
            weight.finish(half, half)

    def finish(name):
        near(name)
        far(name)

    def drain(names):
        for name in names:
            for weight in groups[name]:
                weight.drain()

    in_s = pltpu.make_async_copy(states_s, normed_s, copies.at[0])
    in_h = pltpu.make_async_copy(states_s, hidden, copies.at[1])
    in_t = pltpu.make_async_copy(states_t, normed_t, copies.at[2])
    in_s.start()
    place.barrier(True, True)
    start("P0")
    in_h.start()
    in_t.start()
    in_s.wait()
    normalise(normed_s, gain_s)
    relay("P0", 1)
    start("P1")
    in_t.wait()
    normalise(normed_t, gain_t)
    finish("P0")
    tile = tile_of(sq.shape[1])
    kv_tile = tile_of(kv_width)
    project(normed_s, sk, key_s, cosine, sine, 0, kv_width // kv_tile, kv_tile)
    project(normed_s, sv, value_s, None, None, 0, kv_width // kv_tile, kv_tile)
    project(normed_s, sq, query_s, cosine, sine, 0, sq.shape[1] // tile, tile)
    relay("P1", 1)
    start("P2a")
    start("P2b")
    heads = sq.shape[1] // HD
    group = heads // (kv_width // HD)
    attention(query_s, key_s, value_s, mixed_s, 0, heads, group)
    near("P1")
    in_h.wait()

    count, _, width = own_s.shape
    block_width = map_full.shape[1]
    states_at = pl.ds(pl.multiple_of(place.z * block_width, 128), block_width)
    in_b = pltpu.make_async_copy(
        states_t.at[:, states_at], normed_t.at[:, 0:block_width], copies.at[3]
    )

    steps = ring_order(place.chips)
    per_chip = count // place.chips
    in_order = per_chip * place.chips == count
    if not in_order:
        far("P1")

    def tile_at(j, order):
        if not in_order:
            return j
        turn = lax.div(j, per_chip)
        chip = 0
        for i, step in enumerate(order):
            chip = chip + jnp.where(turn == i, lax.div(place.rep_at(step, 0), 2), 0)
        return chip * per_chip + lax.rem(j, per_chip)

    def produce_s(j):
        return dot_nt(mixed_s[...], so[span(tile_at(j, steps[::-1]), width), :])

    def consume_s(j, total):
        at = span(tile_at(j, steps[::-1]), width)
        hidden[:, at] = (hidden[:, at].astype(F32) + total).astype(BF16)

    t_tile = tile_of(tq.shape[1])
    t_kv = tile_of(tk.shape[1])
    t_heads = tq.shape[1] // HD
    t_group = t_heads // (tk.shape[1] // HD)
    hooks = [(AT["P1"], lambda: far("P1"))] if in_order else []
    hooks += [
        (AT["P2a"], lambda: relay("P2a", 1)),
        (AT["P2b"], lambda: relay("P2b", 1)),
        (AT["P2b"], lambda: start("P3")),
        (AT["P2b near"], lambda: near("P2a")),
        (AT["P2b near"], lambda: near("P2b")),
        (AT["P2a far"], lambda: far("P2a")),
        (AT["P2b far"], lambda: far("P2b")),
    ]
    jobs = []
    for t in range(tk.shape[1] // t_kv):
        jobs.append((tk, key_t, cosine, sine, t, t_kv))
        jobs.append((tv, value_t, None, None, t, t_kv))
    for t in range(tq.shape[1] // t_tile):
        jobs.append((tq, query_t, cosine, sine, t, t_tile))
    tasks = []
    split = len(jobs) <= attn_t.shape[0] and t_kv == t_tile == attn_t.shape[2]
    for i, (weight, out, cos, sin, t, wide_at) in enumerate(jobs):
        if split:
            hooks.append(
                (
                    AT["P2b near"] + i,
                    partial(project_near, place, normed_t, weight, attn_t.at[i], t, wide_at),
                )
            )
            tasks.append(
                partial(
                    project_far, place, normed_t, weight, attn_t.at[i], out, cos, sin, t, wide_at
                )
            )
        else:
            tasks.append(partial(project, normed_t, weight, out, cos, sin, t, 1, wide_at))
    tasks.append(lambda: drain(("P0", "P1", "P2a", "P2b")))
    tasks.append(in_b.start)
    for h in range(t_heads):
        tasks.append(partial(attention, query_t, key_t, value_t, mixed_t, h, 1, t_group))
    hooks += [(AT["P2b far"] + i // 2, task) for i, task in enumerate(tasks)]
    hooks.append((AT["P3"], lambda: relay("P3", 1)))
    hooks.append((AT["P3"], lambda: start("P4")))
    drain_s = line_sum(
        place, count, produce_s, consume_s, own_s, right_s, left_s, sum_send, sum_recv, hooks
    )
    drain_s()
    near("P3")
    by_chip = shards == place.chips
    if not by_chip:
        far("P3")

    per_block, _, width_t = attn_t.shape
    in_b.wait()

    def produce_t(j):
        return dot_nt(mixed_t[...], to[span(j, width_t), :])

    columns = (tk, tv)

    def column_copy(t):
        return pltpu.make_async_copy(
            map_full.at[:, t * width_t : (t + 1) * width_t],
            columns[t % 2].at[0 : map_full.shape[0]],
            map_sems.at[t % 2],
        )

    def first_columns():
        for t in range(min(2, per_block)):
            column_copy(t).start()

    def predict(t):
        column_copy(t).wait()
        product = jnp.dot(
            hidden[...], columns[t % 2][0 : map_full.shape[0]], preferred_element_type=F32
        )
        at = pl.ds(t * width_t, width_t)
        attn_t[t] += normed_t[:, at].astype(F32) - product
        if t + 2 < per_block:
            column_copy(t + 2).start()

    def own_terms():
        for t in range(per_block):
            attn_t[t] += produce_t(place.z * per_block + t).astype(BF16).astype(F32)

    attn_t[...] = jnp.zeros_like(attn_t)
    hooks = [(per_block - 1, lambda: far("P3"))] if by_chip else []
    hooks += [(per_block, own_terms), (AT["P4"], lambda: relay("P4", 1))]
    hooks += [(AT["P4 far"], lambda: finish("P4")), (AT["P4 far"], first_columns)]
    hooks += [(AT["P4 far"] + 1 + t, partial(predict, t)) for t in range(per_block)]
    opposite = lax.div(place.rep_at(half, 0), 2)
    drain_t = line_scatter(
        place, per_block, produce_t, attn_t, opposite if by_chip else place.shards - 1, right_t,
        left_t, scatter_send, scatter_recv, hooks,
    )
    scaling = 1.0 / math.sqrt(reps * length)
    grad_pred = normed_t.at[:, 0:block_width]
    for t in range(per_block):
        grad_pred[:, t * width_t : (t + 1) * width_t] = (attn_t[t] * -scaling).astype(BF16)

    rows = query_grad.shape[0]
    wide = query_grad.shape[1]
    pair_sems = (pair_send, pair_recv)
    ring_sems = (ring_send, ring_recv)

    def ring_sum(index, sums, first, ring, out, columns):
        def pair(i):
            return tq.at[(first + i) * rows : (first + i + 1) * rows, columns]

        def landing(way, m):
            return ring.at[way, m, :, columns]

        return RingScatter(
            place, sums.at[:, columns], pair, landing, out.at[:, columns], index, pair_sems, ring_sems
        )

    parts = 2 if heads % 2 == 0 else 1
    part_wide = wide // parts
    cuts = [slice(c * part_wide, (c + 1) * part_wide) for c in range(parts)]
    out_sum = ring_sum(0, sq, 0, ring_out, out_total, slice(0, wide))
    query_sums = [
        ring_sum(1 + c, so, place.chips, ring_query, query_total, cut) for c, cut in enumerate(cuts)
    ]
    out_copy = pltpu.make_async_copy(out_total, output_grad, copies.at[4])
    query_copies = [
        pltpu.make_async_copy(query_total.at[:, cut], query_grad.at[:, cut], copies.at[5 + c])
        for c, cut in enumerate(cuts)
    ]

    slots = length // width

    def rows_copy(j):
        slot_at = lax.rem(j, slots)
        return pltpu.make_async_copy(
            map_full.at[span(tile_at(j, steps), width)],
            normed_t.at[span(slot_at, width), block_width : 2 * block_width],
            map_sems.at[2 + slot_at],
        )

    def produce_b(j):
        rows_copy(j).wait()
        at = span(lax.rem(j, slots), width)
        product = dot_nt(grad_pred[...], normed_t[at, block_width : 2 * block_width])

        @pl.when(j + slots < count)
        def _():
            rows_copy(j + slots).start()

        return product

    drain(("P3", "P4"))
    grad_mixed[...] = jnp.zeros_like(grad_mixed)
    flips = length <= to.shape[1]

    def consume_b(j, total):
        at = span(tile_at(j, steps), width)
        grad = total.astype(BF16)
        grad_mixed[...] += jnp.dot(grad, so[at, :], preferred_element_type=F32)
        sq[at, :] = dot_tn(grad, mixed_s[...]).astype(BF16)
        if flips:
            to[at, 0:length] = normed_s[:, at].T

    for j in range(min(slots, count)):
        rows_copy(j).start()
    done = []
    for i in range(place.chips):
        ready = (i + 1) * per_chip - 1 if in_order else count
        done.append((ready, partial(out_sum.exchange, i)))
        if i < place.chips - 1:
            done.append((ready + 3 if in_order else count, partial(out_sum.forward, i)))
    drain_b = line_sum(
        place, count, produce_b, consume_b, own_s, right_s, left_s, sum_send, sum_recv, [], done
    )
    grad_query = query_t.at[:, 0:wide]

    def one_head(h, carry):
        backward_head(h, query_s, key_s, value_s, grad_mixed, grad_query, cosine, sine, group)
        return carry

    pending = [lambda: out_sum.forward(place.chips - 1), out_copy.start]
    for c, cut in enumerate(cuts):
        part_heads = heads // parts
        lax.fori_loop(c * part_heads, (c + 1) * part_heads, one_head, 0)
        total = query_sums[c]

        def query_rows(at):
            if flips:
                term = jnp.dot(to[at, 0:length], grad_query[:, cut], preferred_element_type=F32)
            else:
                term = dot_tn(normed_s[:, at], grad_query[:, cut])
            so[at, cut] = term.astype(BF16)

        def query_tile(t, carry):
            query_rows(span(t, width))
            return carry

        if not in_order:
            lax.fori_loop(0, count, query_tile, 0)
        for i, step in enumerate(steps):
            if in_order:
                query_rows(span(lax.div(place.rep_at(step, 0), 2), per_chip * width))
            total.exchange(i)
            if i > 0:
                total.send_fresh(i - 1)
            if pending and i > 0:
                pending.pop(0)()
        total.send_fresh(len(steps) - 1)
        while pending:
            pending.pop(0)()
        pending = [partial(total.send_sums, i) for i in range(1, len(steps))]
        pending.append(query_copies[c].start)
    while pending:
        pending.pop(0)()
    drain_t()
    drain_b()
    out_sum.drain()
    for total in query_sums:
        total.drain()
    out_copy.wait()
    for copy in query_copies:
        copy.wait()


def local(
    reps,
    shards,
    teacher_states,
    student_states,
    teacher_gain,
    student_gain,
    teacher_query,
    teacher_key,
    teacher_value,
    teacher_output,
    student_query,
    student_key,
    student_value,
    student_output,
    projection,
):
    length, d_t = teacher_states.shape
    rows, heads_s = student_query.shape
    d_s = rows * reps
    local_heads = heads_s // HD
    group_size = HQ_S // KV_S
    kv_width = max(local_heads // group_size, 1) * HD

    def kv_start_of(z):
        return lax.div(z * local_heads, group_size) * HD

    cosine, sine = tables(length)
    heads_t = teacher_query.shape[1]
    kv_t = teacher_key.shape[1]
    block_width = projection.shape[1]
    wide_s = 128
    wide_t = tile_of(block_width)
    count_s = d_s // wide_s
    per_block = block_width // wide_t
    most = (shards - 1) * per_block
    chips = reps // 2
    messages = 4 * (chips // 2) + 1
    ring_messages = 1 + 2 * (chips // 2 - 1)
    any_spec = pl.BlockSpec(memory_space=pl.ANY)
    vmem_spec = pl.BlockSpec(memory_space=pltpu.VMEM)
    sds = jax.ShapeDtypeStruct
    dma = pltpu.SemaphoreType.DMA

    def vmem(*shape, dtype=BF16):
        return pltpu.VMEM(shape, dtype)

    _, query_grad, output_grad = pl.pallas_call(
        partial(step_kernel, (reps, shards, kv_start_of)),
        out_shape=(
            sds((d_s, block_width), BF16),
            sds((rows, heads_s), F32),
            sds((rows, heads_s), F32),
        ),
        in_specs=[any_spec] * 2 + [vmem_spec] * 4 + [any_spec] * 9,
        out_specs=(any_spec,) * 3,
        scratch_shapes=[
            vmem(d_s, heads_s),
            vmem(d_s, kv_width),
            vmem(d_s, kv_width),
            vmem(d_s, heads_s),
            vmem(d_t, heads_t),
            vmem(d_t, kv_t),
            vmem(d_t, kv_t),
            vmem(d_t, heads_t),
            vmem(length, d_s),
            vmem(length, d_t),
            vmem(length, d_s),
            vmem(count_s, length, wide_s),
            vmem(count_s, length, wide_s),
            vmem(count_s, length, wide_s),
            vmem(length, heads_s),
            vmem(length, kv_width),
            vmem(length, kv_width),
            vmem(length, heads_s),
            vmem(length, heads_t),
            vmem(length, kv_t),
            vmem(length, kv_t),
            vmem(length, heads_t),
            vmem(per_block, length, wide_t, dtype=F32),
            vmem(most, length, wide_t),
            vmem(most, length, wide_t),
            vmem(length, heads_s, dtype=F32),
            vmem(2, ring_messages, rows // 2, heads_s),
            vmem(2, ring_messages, rows // 2, heads_s),
            vmem(rows, heads_s, dtype=F32),
            vmem(rows, heads_s, dtype=F32),
            dma((9, messages)),
            dma((9, messages)),
            dma((9,)),
            dma((2, count_s)),
            dma((2, count_s)),
            dma((2, most)),
            dma((2, most)),
            dma((3, chips)),
            dma((3, chips)),
            dma((3, 2, ring_messages)),
            dma((3, 2, ring_messages)),
            dma((7,)),
            dma((2 + length // wide_s,)),
        ],
        compiler_params=pltpu.CompilerParams(
            collective_id=0, has_side_effects=True, vmem_limit_bytes=VMEM_BYTES
        ),
    )(
        student_states,
        teacher_states,
        student_gain,
        teacher_gain,
        jnp.asarray(cosine),
        jnp.asarray(sine),
        student_query,
        student_key,
        student_value,
        student_output,
        teacher_query,
        teacher_key,
        teacher_value,
        teacher_output,
        projection,
    )
    return (query_grad, output_grad)


def solution(mesh):
    return jax.shard_map(
        partial(local, mesh.shape["rep"], mesh.shape["shard"]),
        mesh=mesh,
        in_specs=(
            P("rep", None),
            P("rep", None),
            P(),
            P(),
            P("rep", "shard"),
            P("rep", "shard"),
            P("rep", "shard"),
            P("rep", "shard"),
            P("rep", "shard"),
            P("rep", None),
            P("rep", None),
            P("rep", "shard"),
            P("rep", "shard"),
        ),
        out_specs=(P("rep", "shard"), P("rep", "shard")),
        check_vma=False,
    )
```

```python
from functools import partial
import math

import jax
import jax.numpy as jnp
import numpy as np
from jax import lax
from jax.experimental import pallas as pl
from jax.experimental.pallas import tpu as pltpu
from jax.sharding import PartitionSpec as P

HQ_S = 16
KV_S = 4
HD = 128

theta_base = 1000000.0
norm_epsilon = 1e-06

F32 = jnp.float32
BF16 = jnp.bfloat16
VMEM_BYTES = 67_000_000
LAG = 2
AT = {"P1": 10, "P2a": 8, "P2b": 18, "P2b near": 20, "P2a far": 24, "P2b far": 26, "P3": 40, "P4": 9, "P4 far": 13}


def tables(length):
    halfway = HD // 2
    inverse = theta_base ** (-(np.arange(halfway) * 2.0 / HD))
    inverse = inverse.astype(np.float32)
    angles = np.arange(length, dtype=np.float32)[:, None] * inverse[None, :]
    cosine = np.cos(angles)
    sine = np.sin(angles)
    return (
        np.concatenate([cosine, cosine], axis=1).astype(np.float32),
        np.concatenate([-sine, sine], axis=1).astype(np.float32),
    )


def tile_of(width):
    return 256 if width % 256 == 0 else 128


def dot_nt(left, right):
    return lax.dot_general(left, right, (((1,), (1,)), ((), ())), preferred_element_type=F32)


def dot_tn(left, right):
    return lax.dot_general(left, right, (((0,), (0,)), ((), ())), preferred_element_type=F32)


def span(index, size):
    return pl.ds(pl.multiple_of(index * size, size), size)


class Place:
    def __init__(self, reps, shards):
        self.reps = reps
        self.shards = shards
        self.chips = reps // 2
        self.r = lax.axis_index("rep")
        self.z = lax.axis_index("shard")
        chip = lax.div(self.r, 2)
        self.core = lax.rem(self.r, 2)
        row = lax.div(chip, 2)
        self.pos = 2 * row + lax.rem(lax.rem(chip, 2) + row, 2)
        self.partner = 2 * chip + 1 - self.core
        self.right = self.rep_at(1, self.core)
        self.left = self.rep_at(-1, self.core)

    def rep_at(self, step, core):
        place = lax.rem(self.pos + step + self.chips, self.chips)
        row = lax.div(place, 2)
        chip = 2 * row + lax.rem(lax.rem(place, 2) + row, 2)
        return 2 * chip + core

    def barrier(self, ring, line):
        sem = pltpu.get_barrier_semaphore()
        if ring:
            for target in (self.partner, self.left, self.right):
                pl.semaphore_signal(sem, inc=1, device_id={"rep": target})
        if line:

            @pl.when(self.z > 0)
            def _():
                pl.semaphore_signal(sem, inc=1, device_id={"shard": self.z - 1})

            @pl.when(self.z < self.shards - 1)
            def _():
                pl.semaphore_signal(sem, inc=1, device_id={"shard": self.z + 1})

        peers = 3 if ring else 0
        if line:
            peers += jnp.minimum(self.z, 1) + jnp.minimum(self.shards - 1 - self.z, 1)
        pl.semaphore_wait(sem, peers)


class Gather:
    def __init__(self, place, source, full, index, send_sem, recv_sem, local_sem):
        self.place = place
        self.source = source
        self.full = full
        self.index = index
        self.send_sem = send_sem
        self.recv_sem = recv_sem
        self.local_sem = local_sem
        self.rows = source.shape[0]
        self.half = place.chips // 2

    def slab(self, owner, part):
        if part is None:
            return self.full.at[pl.ds(pl.multiple_of(owner * self.rows, self.rows), self.rows)]
        rows = self.rows // 2
        return self.full.at[pl.ds(pl.multiple_of((2 * owner + part) * rows, rows), rows)]

    def copy(self, message, target, owner, part, source=None):
        slab = self.slab(owner, part)
        return pltpu.make_async_remote_copy(
            src_ref=slab if source is None else source,
            dst_ref=slab,
            send_sem=self.send_sem.at[self.index, message],
            recv_sem=self.recv_sem.at[self.index, message],
            device_id={"rep": target},
        )

    def part_of(self, step, way):
        return None if step < self.half else way

    def local(self):
        return pltpu.make_async_copy(
            self.source, self.slab(self.place.r, None), self.local_sem.at[self.index]
        )

    def start(self):
        p = self.place
        h = self.half
        self.copy(0, p.right, p.r, self.part_of(1, 0), self.source).start()
        self.copy(h, p.left, p.r, self.part_of(1, 1), self.source).start()
        self.copy(2 * h, p.partner, p.r, None, self.source).start()
        self.local().start()

    def relay(self, step):
        p = self.place
        h = self.half
        for way, sign, target in ((0, -1, p.right), (1, 1, p.left)):
            owner = p.rep_at(sign * step, p.core)
            base = way * h
            self.copy(base + step - 1, target, owner, self.part_of(step, way)).wait_recv()
            if step < h:
                self.copy(base + step, target, owner, self.part_of(step + 1, way)).start()
            self.copy(2 * h + base + step, p.partner, owner, self.part_of(step, way)).start()

    def finish(self, first, last):
        p = self.place
        h = self.half
        if first == 1:
            self.local().wait()
            self.copy(2 * h, p.partner, p.partner, None).wait_recv()
        for step in range(first, last + 1):
            for way, sign in ((0, -1), (1, 1)):
                owner = p.rep_at(sign * step, 1 - p.core)
                self.copy(
                    2 * h + way * h + step, p.partner, owner, self.part_of(step, way)
                ).wait_recv()

    def drain(self):
        p = self.place
        h = self.half
        for way, sign, target in ((0, -1, p.right), (1, 1, p.left)):
            for step in range(1, h + 1):
                owner = p.rep_at(sign * (step - 1), p.core)
                self.copy(way * h + step - 1, target, owner, self.part_of(step, way)).wait_send()
                owner = p.rep_at(sign * step, p.core)
                self.copy(
                    2 * h + way * h + step, p.partner, owner, self.part_of(step, way)
                ).wait_send()
        self.copy(2 * h, p.partner, p.r, None).wait_send()


def run_hooks(hooks, wave, last):
    for at, action in hooks:
        if at < last:
            pl.when(wave == at)(action)


def late_hooks(hooks, last):
    for at, action in hooks:
        if at >= last:
            action()


def line_sum(place, count, produce, consume, own, rightward, leftward, send_sem, recv_sem, hooks,
             done_hooks=()):
    z = place.z
    ends = place.shards - 1
    waves = count + LAG * ends

    def copy(way, j):
        buffer = (rightward, leftward)[way]
        return pltpu.make_async_remote_copy(
            src_ref=buffer.at[j],
            dst_ref=buffer.at[j],
            send_sem=send_sem.at[way, j],
            recv_sem=recv_sem.at[way, j],
            device_id={"shard": (z + 1, z - 1)[way]},
        )

    def has_before(way):
        return (z > 0, z < ends)[way]

    def has_after(way):
        return (z < ends, z > 0)[way]

    def valid(j):
        return (j >= 0) & (j < count)

    def wave_body(w, carry):
        at = (w - LAG * z, w - LAG * (ends - z))
        first = jnp.maximum(at[0], at[1])
        final = jnp.minimum(at[0], at[1])

        @pl.when(valid(first))
        def _():
            own[first] = produce(first).astype(BF16)

        for way in range(2):
            j = at[way]
            buffer = (rightward, leftward)[way]

            @pl.when(valid(j))
            def _():
                @pl.when(has_before(way))
                def _():
                    copy(way, j).wait_recv()
                    buffer[j] = (own[j].astype(F32) + buffer[j].astype(F32)).astype(BF16)

                @pl.when(jnp.logical_not(has_before(way)))
                def _():
                    buffer[j] = own[j]

                @pl.when(has_after(way))
                def _():
                    copy(way, j).start()

        @pl.when(valid(final))
        def _():
            total = rightward[final].astype(F32) + leftward[final].astype(F32)
            consume(final, total - own[final].astype(F32))
            run_hooks(done_hooks, final, count)

        run_hooks(hooks, w, waves)
        return carry

    lax.fori_loop(0, waves, wave_body, 0)
    late_hooks(hooks, waves)
    late_hooks(done_hooks, count)

    def drain(j, carry):
        for way in range(2):

            @pl.when(has_after(way))
            def _():
                copy(way, j).wait_send()

        return carry

    return lambda: lax.fori_loop(0, count, drain, 0)


def turn_of(u, late):
    return jnp.where((late == 0) & (u < 2), 1 - u, u)


def line_scatter(
    place, per_block, produce, own, late, rightward, leftward, send_sem, recv_sem, hooks
):
    z = place.z
    ends = place.shards - 1
    count = ends * per_block
    waves = count + LAG * ends

    def copy(way, q):
        buffer = (rightward, leftward)[way]
        return pltpu.make_async_remote_copy(
            src_ref=buffer.at[q],
            dst_ref=buffer.at[q],
            send_sem=send_sem.at[way, q],
            recv_sem=recv_sem.at[way, q],
            device_id={"shard": (z + 1, z - 1)[way]},
        )

    def block_at(way, q):
        last = late if way else ends - late
        return turn_of(lax.div(q, per_block), last)

    def wave_body(w, carry):
        for way in range(2):
            line = (z, ends - z)[way]
            q = w - LAG * line
            valid = (q >= 0) & (q < count)
            place_q = jnp.clip(q, 0, count - 1)
            block = block_at(way, place_q)
            chunk = lax.rem(place_q, per_block)
            buffer = (rightward, leftward)[way]
            before = line > 0

            @pl.when(valid & (block < ends - line))
            def _():
                target = (ends - block, block)[way]
                term = produce(target * per_block + chunk).astype(BF16)

                @pl.when(before)
                def _():
                    copy(way, q).wait_recv()
                    buffer[q] = (term.astype(F32) + buffer[q].astype(F32)).astype(BF16)

                @pl.when(jnp.logical_not(before))
                def _():
                    buffer[q] = term

                copy(way, q).start()

            @pl.when(valid & before & (block == ends - line))
            def _():
                copy(way, q).wait_recv()
                own[chunk] += buffer[q].astype(F32)

        run_hooks(hooks, w, waves)
        return carry

    lax.fori_loop(0, waves, wave_body, 0)
    late_hooks(hooks, waves)

    def finish():
        for way in range(2):
            line = (z, ends - z)[way]

            def drain(q, carry):
                @pl.when(block_at(way, q) < ends - line)
                def _():
                    copy(way, q).wait_send()

                return carry

            lax.fori_loop(0, count, drain, 0)

    return finish


class RingScatter:
    def __init__(self, place, partial_sums, pair, ring, out, index, pair_sems, ring_sems):
        self.place = place
        self.partial = partial_sums
        self.pair = pair
        self.ring = ring
        self.out = out
        self.index = index
        self.pair_sems = pair_sems
        self.ring_sems = ring_sems
        self.half = place.chips // 2
        self.rows = out.shape[0]
        self.steps = ring_order(place.chips)

    def exchange(self, i):
        self.pair_copy(i).start()

    def pair_copy(self, i):
        owner = self.place.rep_at(self.steps[i], 1 - self.place.core)
        return pltpu.make_async_remote_copy(
            src_ref=self.partial.at[span(owner, self.rows)],
            dst_ref=self.pair(i),
            send_sem=self.pair_sems[0].at[self.index, i],
            recv_sem=self.pair_sems[1].at[self.index, i],
            device_id={"rep": self.place.partner},
        )

    def message(self, step, part):
        return 0 if step == self.half else 1 + 2 * (self.half - 1 - step) + part

    def half_of(self, ref, part):
        return ref.at[pl.ds(part * (self.rows // 2), self.rows // 2)]

    def ring_copy(self, way, step, part, i):
        m = self.message(step, part)
        return pltpu.make_async_remote_copy(
            src_ref=self.half_of(self.pair(i), part),
            dst_ref=self.ring(way, m),
            send_sem=self.ring_sems[0].at[self.index, way, m],
            recv_sem=self.ring_sems[1].at[self.index, way, m],
            device_id={"rep": (self.place.right, self.place.left)[way]},
        )

    def moves(self, i):
        e, h = self.steps[i], self.half
        if e == h:
            return [(way, h, way, False) for way in range(2)]
        way, step = (0, e) if e > 0 else (1, -e)
        return [(way, step, part, part == way or step + 1 < h) for part in range(2)]

    def fresh(self, i, part):
        owner = self.place.rep_at(self.steps[i], self.place.core)
        rows = self.rows // 2
        mine = self.partial[span(2 * owner + part, rows), :].astype(F32)
        return mine + self.half_of(self.pair(i), part)[...].astype(F32)

    def incoming(self, way, step, part, i):
        self.ring_copy(way, step, part, i).wait_recv()
        return self.ring(way, self.message(step, part))[...].astype(F32)

    def send(self, i, summed):
        for way, step, part, has in self.moves(i):
            if has == summed:
                value = self.fresh(i, part)
                if has:
                    value = value + self.incoming(way, step + 1, part, i)
                self.half_of(self.pair(i), part)[...] = value.astype(BF16)
                self.ring_copy(way, step, part, i).start()

    def send_fresh(self, i):
        self.pair_copy(i).wait_recv()
        if self.steps[i] != 0:
            self.send(i, False)

    def send_sums(self, i):
        if self.steps[i] != 0:
            self.send(i, True)
            return
        for part in range(2):
            value = self.fresh(i, part)
            for way in range(2):
                if part == way or self.half > 1:
                    value = value + self.incoming(way, 1, part, i)
            self.half_of(self.out, part)[...] = value

    def forward(self, i):
        self.send_fresh(i)
        self.send_sums(i)

    def drain(self):
        for i, e in enumerate(self.steps):
            self.pair_copy(i).wait_send()
            if e != 0:
                for way, step, part, _ in self.moves(i):
                    self.ring_copy(way, step, part, i).wait_send()


def ring_order(chips):
    half = chips // 2
    order = [half]
    for step in range(half - 1, 0, -1):
        order += [step, -step]
    return order + [0]


def normalise(states, gain, block=16):
    length, width = states.shape

    def body(i, carry):
        at = pl.ds(pl.multiple_of(i * block, block), block)
        rows = states[at, :].astype(F32)
        meansq = jnp.sum(rows * rows, axis=-1, keepdims=True) * (1.0 / width)
        states[at, :] = (rows * lax.rsqrt(meansq + norm_epsilon) * gain[...][None, :]).astype(BF16)
        return carry

    lax.fori_loop(0, length // block, body, 0)


def turned(values, cosine, sine):
    return values * cosine + pltpu.roll(values, HD // 2, 1) * sine


def project(normed, weight, out, cosine, sine, first, count, tile):
    def body(t, carry):
        at = pl.ds(pl.multiple_of(t * tile, tile), tile)
        value = jnp.dot(normed[...], weight[:, at], preferred_element_type=F32)
        if cosine is None:
            out[:, at] = value.astype(BF16)
        else:
            for head in range(tile // HD):
                part = turned(value[:, head * HD : (head + 1) * HD], cosine[...], sine[...])
                spot = pl.ds(pl.multiple_of(t * tile + head * HD, HD), HD)
                out[:, spot] = part.astype(BF16)
        return carry

    lax.fori_loop(first, first + count, body, 0)


def project_near(place, normed, weight, total, t, tile):
    at = span(t, tile)
    size = weight.shape[0] // place.chips
    value = None
    for step in ring_order(place.chips)[1:]:
        rows = span(lax.div(place.rep_at(step, 0), 2), size)
        term = jnp.dot(normed[:, rows], weight[rows, at], preferred_element_type=F32)
        value = term if value is None else value + term
    total[...] = value


def project_far(place, normed, weight, total, out, cosine, sine, t, tile):
    at = span(t, tile)
    size = weight.shape[0] // place.chips
    rows = span(lax.div(place.rep_at(place.chips // 2, 0), 2), size)
    value = total[...] + jnp.dot(normed[:, rows], weight[rows, at], preferred_element_type=F32)
    if cosine is None:
        out[:, at] = value.astype(BF16)
    else:
        for head in range(tile // HD):
            part = turned(value[:, head * HD : (head + 1) * HD], cosine[...], sine[...])
            out[:, t * tile + head * HD : t * tile + (head + 1) * HD] = part.astype(BF16)


def soft(scores):
    highest = jnp.max(scores, axis=-1, keepdims=True)
    weights = jnp.exp(scores - highest)
    return weights / jnp.sum(weights, axis=-1, keepdims=True)


def masked_scores(query, keys):
    scores = dot_nt(query, keys) * HD ** (-0.5)
    row = lax.broadcasted_iota(jnp.int32, scores.shape, 0)
    column = lax.broadcasted_iota(jnp.int32, scores.shape, 1)
    return jnp.where(row >= column, scores, -1e30)


def attention(queries, keys, values, mixed, first, count, group):
    def body(h, carry):
        at = pl.ds(pl.multiple_of(h * HD, HD), HD)
        kv = pl.ds(pl.multiple_of(lax.div(h, group) * HD, HD), HD)
        probs = soft(masked_scores(queries[:, at], keys[:, kv])).astype(BF16)
        mixed[:, at] = jnp.dot(probs, values[:, kv], preferred_element_type=F32).astype(BF16)
        return carry

    lax.fori_loop(first, first + count, body, 0)


def backward_head(h, query, keys, values, grad_mixed, grad_query, cosine, sine, group):
    at = span(h, HD)
    kv = span(lax.div(h, group), HD)
    probs = soft(masked_scores(query[:, at], keys[:, kv]))
    grad_probs = dot_nt(grad_mixed[:, at].astype(BF16), values[:, kv]).astype(BF16).astype(F32)
    inner = jnp.sum(grad_probs * probs, axis=-1, keepdims=True)
    grad_scores = probs * (grad_probs - inner) * HD ** (-0.5)
    grad_rot = jnp.dot(grad_scores.astype(BF16), keys[:, kv], preferred_element_type=F32)
    grad_rot = grad_rot.astype(BF16).astype(F32)
    grad_query[:, at] = turned(grad_rot, cosine[...], -sine[...]).astype(BF16)


def step_kernel(
    sizes,
    states_s,
    states_t,
    gain_s,
    gain_t,
    cosine,
    sine,
    w_sq,
    w_sk,
    w_sv,
    w_so,
    w_tq,
    w_tk,
    w_tv,
    w_to,
    w_pj,
    map_full,
    query_grad,
    output_grad,
    sq,
    sk,
    sv,
    so,
    tq,
    tk,
    tv,
    to,
    normed_s,
    normed_t,
    hidden,
    own_s,
    right_s,
    left_s,
    query_s,
    key_s,
    value_s,
    mixed_s,
    query_t,
    key_t,
    value_t,
    mixed_t,
    attn_t,
    right_t,
    left_t,
    grad_mixed,
    ring_out,
    ring_query,
    query_total,
    out_total,
    gather_send,
    gather_recv,
    gather_local,
    sum_send,
    sum_recv,
    scatter_send,
    scatter_recv,
    pair_send,
    pair_recv,
    ring_send,
    ring_recv,
    copies,
    map_sems,
):
    reps, shards, kv_start_of = sizes
    place = Place(reps, shards)
    length = normed_s.shape[0]
    kv_width = sk.shape[1]
    kv_at = pl.ds(pl.multiple_of(kv_start_of(place.z), HD), kv_width)
    sources = (w_sq, w_sk.at[:, kv_at], w_sv.at[:, kv_at], w_so, w_tq, w_tk, w_tv, w_to, w_pj)
    fulls = (sq, sk, sv, so, tq, tk, tv, to, map_full)
    weights = [
        Gather(place, source, full, i, gather_send, gather_recv, gather_local)
        for i, (source, full) in enumerate(zip(sources, fulls))
    ]
    half = place.chips // 2
    groups = {
        "P0": weights[0:3],
        "P1": weights[3:4],
        "P2a": weights[5:7],
        "P2b": weights[4:5],
        "P3": weights[7:8],
        "P4": weights[8:9],
    }

    def start(name):
        for weight in groups[name]:
            weight.start()

    def relay(name, step):
        for weight in groups[name]:
            weight.relay(step)

    def near(name):
        for step in range(2, half):
            relay(name, step)
        for weight in groups[name]:
            weight.finish(1, half - 1)

    def far(name):
        relay(name, half)
        for weight in groups[name]:
            weight.finish(half, half)

    def finish(name):
        near(name)
        far(name)

    def drain(names):
        for name in names:
            for weight in groups[name]:
                weight.drain()

    in_s = pltpu.make_async_copy(states_s, normed_s, copies.at[0])
    in_h = pltpu.make_async_copy(states_s, hidden, copies.at[1])
    in_t = pltpu.make_async_copy(states_t, normed_t, copies.at[2])
    in_s.start()
    place.barrier(True, True)
    start("P0")
    in_h.start()
    in_t.start()
    in_s.wait()
    normalise(normed_s, gain_s)
    relay("P0", 1)
    start("P1")
    in_t.wait()
    normalise(normed_t, gain_t)
    finish("P0")
    tile = tile_of(sq.shape[1])
    kv_tile = tile_of(kv_width)
    project(normed_s, sk, key_s, cosine, sine, 0, kv_width // kv_tile, kv_tile)
    project(normed_s, sv, value_s, None, None, 0, kv_width // kv_tile, kv_tile)
    project(normed_s, sq, query_s, cosine, sine, 0, sq.shape[1] // tile, tile)
    relay("P1", 1)
    start("P2a")
    start("P2b")
    heads = sq.shape[1] // HD
    group = heads // (kv_width // HD)
    attention(query_s, key_s, value_s, mixed_s, 0, heads, group)
    near("P1")
    in_h.wait()

    count, _, width = own_s.shape
    block_width = map_full.shape[1]
    states_at = pl.ds(pl.multiple_of(place.z * block_width, 128), block_width)
    in_b = pltpu.make_async_copy(
        states_t.at[:, states_at], normed_t.at[:, 0:block_width], copies.at[3]
    )

    steps = ring_order(place.chips)
    per_chip = count // place.chips
    in_order = per_chip * place.chips == count
    if not in_order:
        far("P1")

    def tile_at(j, order):
        if not in_order:
            return j
        turn = lax.div(j, per_chip)
        chip = 0
        for i, step in enumerate(order):
            chip = chip + jnp.where(turn == i, lax.div(place.rep_at(step, 0), 2), 0)
        return chip * per_chip + lax.rem(j, per_chip)

    def produce_s(j):
        return dot_nt(mixed_s[...], so[span(tile_at(j, steps[::-1]), width), :])

    def consume_s(j, total):
        at = span(tile_at(j, steps[::-1]), width)
        hidden[:, at] = (hidden[:, at].astype(F32) + total).astype(BF16)

    t_tile = tile_of(tq.shape[1])
    t_kv = tile_of(tk.shape[1])
    t_heads = tq.shape[1] // HD
    t_group = t_heads // (tk.shape[1] // HD)
    hooks = [(AT["P1"], lambda: far("P1"))] if in_order else []
    hooks += [
        (AT["P2a"], lambda: relay("P2a", 1)),
        (AT["P2b"], lambda: relay("P2b", 1)),
        (AT["P2b"], lambda: start("P3")),
        (AT["P2b near"], lambda: near("P2a")),
        (AT["P2b near"], lambda: near("P2b")),
        (AT["P2a far"], lambda: far("P2a")),
        (AT["P2b far"], lambda: far("P2b")),
    ]
    jobs = []
    for t in range(tk.shape[1] // t_kv):
        jobs.append((tk, key_t, cosine, sine, t, t_kv))
        jobs.append((tv, value_t, None, None, t, t_kv))
    for t in range(tq.shape[1] // t_tile):
        jobs.append((tq, query_t, cosine, sine, t, t_tile))
    tasks = []
    split = len(jobs) <= attn_t.shape[0] and t_kv == t_tile == attn_t.shape[2]
    for i, (weight, out, cos, sin, t, wide_at) in enumerate(jobs):
        if split:
            hooks.append(
                (
                    AT["P2b near"] + i,
                    partial(project_near, place, normed_t, weight, attn_t.at[i], t, wide_at),
                )
            )
            tasks.append(
                partial(
                    project_far, place, normed_t, weight, attn_t.at[i], out, cos, sin, t, wide_at
                )
            )
        else:
            tasks.append(partial(project, normed_t, weight, out, cos, sin, t, 1, wide_at))
    tasks.append(lambda: drain(("P0", "P1", "P2a", "P2b")))
    tasks.append(in_b.start)
    for h in range(t_heads):
        tasks.append(partial(attention, query_t, key_t, value_t, mixed_t, h, 1, t_group))
    hooks += [(AT["P2b far"] + i // 2, task) for i, task in enumerate(tasks)]
    hooks.append((AT["P3"], lambda: relay("P3", 1)))
    hooks.append((AT["P3"], lambda: start("P4")))
    drain_s = line_sum(
        place, count, produce_s, consume_s, own_s, right_s, left_s, sum_send, sum_recv, hooks
    )
    drain_s()
    near("P3")
    by_chip = shards == place.chips
    if not by_chip:
        far("P3")

    per_block, _, width_t = attn_t.shape
    in_b.wait()

    def produce_t(j):
        return dot_nt(mixed_t[...], to[span(j, width_t), :])

    columns = (tk, tv)

    def column_copy(t):
        return pltpu.make_async_copy(
            map_full.at[:, t * width_t : (t + 1) * width_t],
            columns[t % 2].at[0 : map_full.shape[0]],
            map_sems.at[t % 2],
        )

    def first_columns():
        for t in range(min(2, per_block)):
            column_copy(t).start()

    def predict(t):
        column_copy(t).wait()
        product = jnp.dot(
            hidden[...], columns[t % 2][0 : map_full.shape[0]], preferred_element_type=F32
        )
        at = pl.ds(t * width_t, width_t)
        attn_t[t] += normed_t[:, at].astype(F32) - product
        if t + 2 < per_block:
            column_copy(t + 2).start()

    def own_terms():
        for t in range(per_block):
            attn_t[t] += produce_t(place.z * per_block + t).astype(BF16).astype(F32)

    attn_t[...] = jnp.zeros_like(attn_t)
    hooks = [(per_block - 1, lambda: far("P3"))] if by_chip else []
    hooks += [(per_block, own_terms), (AT["P4"], lambda: relay("P4", 1))]
    hooks += [(AT["P4 far"], lambda: finish("P4")), (AT["P4 far"], first_columns)]
    hooks += [(AT["P4 far"] + 1 + t, partial(predict, t)) for t in range(per_block)]
    opposite = lax.div(place.rep_at(half, 0), 2)
    drain_t = line_scatter(
        place, per_block, produce_t, attn_t, opposite if by_chip else place.shards - 1, right_t,
        left_t, scatter_send, scatter_recv, hooks,
    )
    scaling = 1.0 / math.sqrt(reps * length)
    grad_pred = normed_t.at[:, 0:block_width]
    for t in range(per_block):
        grad_pred[:, t * width_t : (t + 1) * width_t] = (attn_t[t] * -scaling).astype(BF16)

    rows = query_grad.shape[0]
    wide = query_grad.shape[1]
    pair_sems = (pair_send, pair_recv)
    ring_sems = (ring_send, ring_recv)

    def ring_sum(index, sums, first, ring, out, columns):
        def pair(i):
            return tq.at[(first + i) * rows : (first + i + 1) * rows, columns]

        def landing(way, m):
            return ring.at[way, m, :, columns]

        return RingScatter(
            place, sums.at[:, columns], pair, landing, out.at[:, columns], index, pair_sems, ring_sems
        )

    parts = 2 if heads % 2 == 0 else 1
    part_wide = wide // parts
    cuts = [slice(c * part_wide, (c + 1) * part_wide) for c in range(parts)]
    out_sum = ring_sum(0, sq, 0, ring_out, out_total, slice(0, wide))
    query_sums = [
        ring_sum(1 + c, so, place.chips, ring_query, query_total, cut) for c, cut in enumerate(cuts)
    ]
    out_copy = pltpu.make_async_copy(out_total, output_grad, copies.at[4])
    query_copies = [
        pltpu.make_async_copy(query_total.at[:, cut], query_grad.at[:, cut], copies.at[5 + c])
        for c, cut in enumerate(cuts)
    ]

    slots = length // width

    def rows_copy(j):
        slot_at = lax.rem(j, slots)
        return pltpu.make_async_copy(
            map_full.at[span(tile_at(j, steps), width)],
            normed_t.at[span(slot_at, width), block_width : 2 * block_width],
            map_sems.at[2 + slot_at],
        )

    def produce_b(j):
        rows_copy(j).wait()
        at = span(lax.rem(j, slots), width)
        product = dot_nt(grad_pred[...], normed_t[at, block_width : 2 * block_width])

        @pl.when(j + slots < count)
        def _():
            rows_copy(j + slots).start()

        return product

    drain(("P3", "P4"))
    grad_mixed[...] = jnp.zeros_like(grad_mixed)
    flips = length <= to.shape[1]

    def consume_b(j, total):
        at = span(tile_at(j, steps), width)
        grad = total.astype(BF16)
        grad_mixed[...] += jnp.dot(grad, so[at, :], preferred_element_type=F32)
        sq[at, :] = dot_tn(grad, mixed_s[...]).astype(BF16)
        if flips:
            to[at, 0:length] = normed_s[:, at].T

    for j in range(min(slots, count)):
        rows_copy(j).start()
    done = []
    for i in range(place.chips):
        ready = (i + 1) * per_chip - 1 if in_order else count
        done.append((ready, partial(out_sum.exchange, i)))
        if i < place.chips - 1:
            done.append((ready + 3 if in_order else count, partial(out_sum.forward, i)))
    drain_b = line_sum(
        place, count, produce_b, consume_b, own_s, right_s, left_s, sum_send, sum_recv, [], done
    )
    grad_query = query_t.at[:, 0:wide]

    def one_head(h, carry):
        backward_head(h, query_s, key_s, value_s, grad_mixed, grad_query, cosine, sine, group)
        return carry

    pending = [lambda: out_sum.forward(place.chips - 1), out_copy.start]
    for c, cut in enumerate(cuts):
        part_heads = heads // parts
        lax.fori_loop(c * part_heads, (c + 1) * part_heads, one_head, 0)
        total = query_sums[c]

        def query_rows(at):
            if flips:
                term = jnp.dot(to[at, 0:length], grad_query[:, cut], preferred_element_type=F32)
            else:
                term = dot_tn(normed_s[:, at], grad_query[:, cut])
            so[at, cut] = term.astype(BF16)

        def query_tile(t, carry):
            query_rows(span(t, width))
            return carry

        if not in_order:
            lax.fori_loop(0, count, query_tile, 0)
        for i, step in enumerate(steps):
            if in_order:
                query_rows(span(lax.div(place.rep_at(step, 0), 2), per_chip * width))
            total.exchange(i)
            if i > 0:
                total.send_fresh(i - 1)
            if pending and i > 0:
                pending.pop(0)()
        total.send_fresh(len(steps) - 1)
        while pending:
            pending.pop(0)()
        pending = [partial(total.send_sums, i) for i in range(1, len(steps))]
        pending.append(query_copies[c].start)
    while pending:
        pending.pop(0)()
    drain_t()
    drain_b()
    out_sum.drain()
    for total in query_sums:
        total.drain()
    out_copy.wait()
    for copy in query_copies:
        copy.wait()


def place_kernel(query_from, output_from, query_to, output_to, query_held, output_held, sems):
    moves = []
    for i, (source, held, target) in enumerate(
        ((query_from, query_held, query_to), (output_from, output_held, output_to))
    ):
        moves.append(pltpu.make_async_copy(source, held, sems.at[i]))
        moves.append(pltpu.make_async_copy(held, target, sems.at[2 + i]))
    moves[0].start()
    moves[2].start()
    moves[0].wait()
    moves[1].start()
    moves[2].wait()
    moves[3].start()
    moves[1].wait()
    moves[3].wait()


def local(
    reps,
    shards,
    teacher_states,
    student_states,
    teacher_gain,
    student_gain,
    teacher_query,
    teacher_key,
    teacher_value,
    teacher_output,
    student_query,
    student_key,
    student_value,
    student_output,
    projection,
):
    length, d_t = teacher_states.shape
    rows, heads_s = student_query.shape
    d_s = rows * reps
    local_heads = heads_s // HD
    group_size = HQ_S // KV_S
    kv_width = max(local_heads // group_size, 1) * HD

    def kv_start_of(z):
        return lax.div(z * local_heads, group_size) * HD

    cosine, sine = tables(length)
    heads_t = teacher_query.shape[1]
    kv_t = teacher_key.shape[1]
    block_width = projection.shape[1]
    wide_s = 128
    wide_t = tile_of(block_width)
    count_s = d_s // wide_s
    per_block = block_width // wide_t
    most = (shards - 1) * per_block
    chips = reps // 2
    messages = 4 * (chips // 2) + 1
    ring_messages = 1 + 2 * (chips // 2 - 1)
    any_spec = pl.BlockSpec(memory_space=pl.ANY)
    vmem_spec = pl.BlockSpec(memory_space=pltpu.VMEM)
    sds = jax.ShapeDtypeStruct
    dma = pltpu.SemaphoreType.DMA

    def vmem(*shape, dtype=BF16):
        return pltpu.VMEM(shape, dtype)

    _, query_grad, output_grad = pl.pallas_call(
        partial(step_kernel, (reps, shards, kv_start_of)),
        out_shape=(
            sds((d_s, block_width), BF16),
            sds((rows, heads_s), F32),
            sds((rows, heads_s), F32),
        ),
        in_specs=[any_spec] * 2 + [vmem_spec] * 4 + [any_spec] * 9,
        out_specs=(any_spec,) * 3,
        scratch_shapes=[
            vmem(d_s, heads_s),
            vmem(d_s, kv_width),
            vmem(d_s, kv_width),
            vmem(d_s, heads_s),
            vmem(d_t, heads_t),
            vmem(d_t, kv_t),
            vmem(d_t, kv_t),
            vmem(d_t, heads_t),
            vmem(length, d_s),
            vmem(length, d_t),
            vmem(length, d_s),
            vmem(count_s, length, wide_s),
            vmem(count_s, length, wide_s),
            vmem(count_s, length, wide_s),
            vmem(length, heads_s),
            vmem(length, kv_width),
            vmem(length, kv_width),
            vmem(length, heads_s),
            vmem(length, heads_t),
            vmem(length, kv_t),
            vmem(length, kv_t),
            vmem(length, heads_t),
            vmem(per_block, length, wide_t, dtype=F32),
            vmem(most, length, wide_t),
            vmem(most, length, wide_t),
            vmem(length, heads_s, dtype=F32),
            vmem(2, ring_messages, rows // 2, heads_s),
            vmem(2, ring_messages, rows // 2, heads_s),
            vmem(rows, heads_s, dtype=F32),
            vmem(rows, heads_s, dtype=F32),
            dma((9, messages)),
            dma((9, messages)),
            dma((9,)),
            dma((2, count_s)),
            dma((2, count_s)),
            dma((2, most)),
            dma((2, most)),
            dma((3, chips)),
            dma((3, chips)),
            dma((3, 2, ring_messages)),
            dma((3, 2, ring_messages)),
            dma((7,)),
            dma((2 + length // wide_s,)),
        ],
        compiler_params=pltpu.CompilerParams(
            collective_id=0, has_side_effects=True, vmem_limit_bytes=VMEM_BYTES
        ),
    )(
        student_states,
        teacher_states,
        student_gain,
        teacher_gain,
        jnp.asarray(cosine),
        jnp.asarray(sine),
        student_query,
        student_key,
        student_value,
        student_output,
        teacher_query,
        teacher_key,
        teacher_value,
        teacher_output,
        projection,
    )
    return pl.pallas_call(
        place_kernel,
        out_shape=(sds((rows, heads_s), F32),) * 2,
        in_specs=[any_spec] * 2,
        out_specs=(any_spec,) * 2,
        scratch_shapes=[vmem(rows, heads_s, dtype=F32)] * 2 + [dma((4,))],
    )(query_grad, output_grad)


def solution(mesh):
    return jax.shard_map(
        partial(local, mesh.shape["rep"], mesh.shape["shard"]),
        mesh=mesh,
        in_specs=(
            P("rep", None),
            P("rep", None),
            P(),
            P(),
            P("rep", "shard"),
            P("rep", "shard"),
            P("rep", "shard"),
            P("rep", "shard"),
            P("rep", "shard"),
            P("rep", None),
            P("rep", None),
            P("rep", "shard"),
            P("rep", "shard"),
        ),
        out_specs=(P("rep", "shard"), P("rep", "shard")),
        check_vma=False,
    )
```
